16 devices in a mesh: rep: 2 (over y, z), dp: 8 (over x, core).
Axes of the slice: x: 4, y: 2, z: 1, core: 2. Of those that a mesh axis runs over, the one named last changes fastest.
The devices are a block of a 4x4x8 slice.
Arguments:
- g_w_gate: bfloat16 [16, 2, 512, 4096], P(('rep', 'dp')), parts along dimension 0
- g_w_up: bfloat16 [16, 2, 512, 4096], P(('rep', 'dp')), parts along dimension 0
- g_w_down: bfloat16 [16, 2, 4096, 512], P(('rep', 'dp')), parts along dimension 0
- w_gate: bfloat16 [2, 512, 4096], replicated
- w_up: bfloat16 [2, 512, 4096], replicated
- w_down: bfloat16 [2, 4096, 512], replicated
- m_w_gate: float32 [2, 512, 4096], P(None, 'dp')
- m_w_up: float32 [2, 512, 4096], P(None, 'dp')
- m_w_down: float32 [2, 4096, 512], P(None, 'dp')
- v_w_gate: float32 [2, 512, 4096], P(None, 'dp')
- v_w_up: float32 [2, 512, 4096], P(None, 'dp')
- v_w_down: float32 [2, 4096, 512], P(None, 'dp')
Outputs:
- output 1: bfloat16 [4, 512, 4096], P('rep'), parts along dimension 0
- output 2: bfloat16 [4, 512, 4096], P('rep'), parts along dimension 0
- output 3: bfloat16 [4, 4096, 512], P('rep'), parts along dimension 0
- output 4: float32 [4, 512, 4096], P('rep', 'dp'), parts along dimension 0
- output 5: float32 [4, 512, 4096], P('rep', 'dp'), parts along dimension 0
- output 6: float32 [4, 4096, 512], P('rep', 'dp'), parts along dimension 0
- output 7: float32 [4, 512, 4096], P('rep', 'dp'), parts along dimension 0
- output 8: float32 [4, 512, 4096], P('rep', 'dp'), parts along dimension 0
- output 9: float32 [4, 4096, 512], P('rep', 'dp'), parts along dimension 0
There are 2 independent parts. The reference program is written for one: setup_inputs(seed, part) draws one part's arguments, and reference() takes and returns one part's arrays. A program takes and returns all parts, laid end to end along the dimension named above; an argument that names none is the same for every part.
All inputs are finite; a program needn't handle non-finite values.
Results may differ from the reference program's by a relative error of at most 0.022.
Values are sent between devices in bfloat16 or wider.
A program may use at most 768 MiB of HBM per device.

```python
import jax
import jax.numpy as jnp
from jax import lax

DEVICES = 8
D = 512
FF = 4096
LAYERS = 2
NAMES = ("w_gate", "w_up", "w_down")
SHAPES = {"w_gate": (LAYERS, D, FF), "w_up": (LAYERS, D, FF), "w_down": (LAYERS, FF, D)}


def setup_inputs(seed: int = 0, part: int = 0) -> dict:
    kz, *keys = jax.random.split(jax.random.key(seed), 1 + 5 * len(NAMES))
    loud = 2.0 ** jax.random.uniform(kz, (), jnp.float32, -1.0, 1.0)
    drawn = {}
    for name, key, both in zip(NAMES, keys[:3], keys[3:6], strict=True):
        own = jax.random.normal(jax.random.fold_in(key, part), (DEVICES, *SHAPES[name]), jnp.float32)
        shared = jax.random.normal(jax.random.fold_in(both, part), SHAPES[name], jnp.float32)
        drawn["g_" + name] = (loud * (0.7 * shared / DEVICES + 0.7 * own * DEVICES**-0.5)).astype(jnp.bfloat16)
    for name, key in zip(NAMES, keys[6:9], strict=True):
        drawn[name] = (jax.random.normal(key, SHAPES[name], jnp.float32) * SHAPES[name][1] ** -0.5).astype(jnp.bfloat16)
    for name, key in zip(NAMES, keys[9:12], strict=True):
        drawn["m_" + name] = loud * 0.5 * jax.random.normal(key, SHAPES[name], jnp.float32)
    for name, key in zip(NAMES, keys[12:15], strict=True):
        drawn["v_" + name] = loud * loud * jax.random.uniform(key, SHAPES[name], jnp.float32, 0.5, 1.5)
    return drawn


def adamw(w, m, v, g):
    m = 0.9 * m + 0.1 * g
    v = 0.95 * v + 0.05 * g * g
    step = m * lax.rsqrt(v + 1e-8) + 0.1 * w
    return (w - 0.02 * step).astype(jnp.bfloat16), m, v


def clipped(gradients, sum_of_squares, count):
    factor = jnp.minimum(1.0, 0.5 * lax.rsqrt(sum_of_squares / count + 1e-30))
    return [g * factor for g in gradients]


def reference(g_w_gate, g_w_up, g_w_down, w_gate, w_up, w_down, m_w_gate, m_w_up, m_w_down, v_w_gate, v_w_up, v_w_down):
    def total(terms):
        return lax.scan(lambda so_far, term: (so_far + term.astype(jnp.float32), None), jnp.zeros(terms.shape[1:], jnp.float32), terms)[0]

    gradients = [total(terms).astype(jnp.bfloat16).astype(jnp.float32) for terms in (g_w_gate, g_w_up, g_w_down)]
    gradients = clipped(gradients, sum(jnp.sum(g * g) for g in gradients), sum(g.size for g in gradients))
    new = [
        adamw(w.astype(jnp.float32), m, v, g)
        for w, m, v, g in zip((w_gate, w_up, w_down), (m_w_gate, m_w_up, m_w_down), (v_w_gate, v_w_up, v_w_down), gradients, strict=True)
    ]
    return tuple(one[which] for which in range(3) for one in new)
```

```python
import functools

import jax
import jax.numpy as jnp
from jax import lax
from jax.experimental import pallas as pl
from jax.experimental.pallas import tpu as pltpu
from jax.sharding import PartitionSpec as P

MESH = pl.DeviceIdType.MESH
CORES = 2
PIECES = 4
TILE = (16, 512)
WAYS = (0, 1)
F32, BF16 = jnp.float32, jnp.bfloat16


def kernel(n, *refs):
    g, w, m_in, v_in, new, m, v = (refs[i : i + 3] for i in range(0, 21, 3))
    far, near, own_w = (refs[i : i + 3] for i in range(21, 30, 3))
    (acc, squares, term_sem, mate_sem, state_sem, far_sem, near_sem, ring_sem, ringfar_sem,
     back_sem, mate_send, back_send, sum_send, ring_send, square_send, square_sem) = refs[30:]

    chips = n // CORES
    me = lax.axis_index("dp")
    chip, core = me // CORES, me % CORES
    mate = chip * CORES + 1 - core
    right_chip, left_chip = lax.rem(chip + 1, chips), lax.rem(chip + chips - 1, chips)
    far_chip = lax.rem(chip + 2, chips)
    side = (right_chip * CORES + core, left_chip * CORES + core)
    arrays = range(3)
    layers = m[0].shape[0]
    half = layers // 2
    block_rows = [ref.shape[1] for ref in m]
    piece_rows = [r // PIECES for r in block_rows]
    steps = [(a, l) for l in range(half) for a in arrays]

    def rows(a, block, q):
        return pl.ds(pl.multiple_of(block * block_rows[a] + q * piece_rows[a], piece_rows[a]), piece_rows[a])

    def to(device):
        return {"device_id": {"dp": device}, "device_id_type": MESH}

    def mine(c):
        return c * CORES + core

    def mates(c):
        return c * CORES + 1 - core

    def tiles(a):
        columns = m[a].shape[2] // TILE[1]
        count = piece_rows[a] // TILE[0] * columns

        def at(i, base):
            r = pl.multiple_of(base + i // columns * TILE[0], TILE[0])
            c = pl.multiple_of(i % columns * TILE[1], TILE[1])
            return pl.ds(r, TILE[0]), pl.ds(c, TILE[1])

        return count, at

    targets = (far_chip, right_chip, left_chip, chip)
    places = [(t, a, layer) for t in range(4) for a in arrays for layer in range(layers)]

    def term(t, a, layer, q):
        where = rows(a, mine(targets[t]), q)
        return pltpu.make_async_copy(g[a].at[0, layer, where, :], new[a].at[layer, where, :], term_sem.at[t, a, layer, q])

    def mate_term(t, a, layer, q):
        theirs = new[a].at[layer, rows(a, mine(targets[t]), q), :]
        return pltpu.make_async_remote_copy(
            src_ref=g[a].at[0, layer, rows(a, mates(targets[t]), q), :], dst_ref=theirs,
            send_sem=mate_send.at[a], recv_sem=mate_sem.at[t, a, layer, q], **to(mate))

    def states(a):
        own = pl.ds(pl.multiple_of(me * block_rows[a], block_rows[a]), block_rows[a])
        return (pltpu.make_async_copy(m_in[a], m[a], state_sem.at[0, a]),
                pltpu.make_async_copy(v_in[a], v[a], state_sem.at[1, a]),
                pltpu.make_async_copy(w[a].at[:, own, :], own_w[a], state_sem.at[2, a]))

    barrier = pltpu.get_barrier_semaphore()
    for o in range(1, n):
        pl.semaphore_signal(barrier, inc=1, **to(lax.rem(me + o, n)))
    for t, a, layer in places[: 3 * layers]:
        @pl.loop(0, PIECES)
        def _(q):
            term(t, a, layer, q).start()
    pl.semaphore_wait(barrier, n - 1)

    order = [(t, a, layer) for t in range(4) for a, l in steps for layer in (l, half + l)]
    for t, a, layer in order:
        @pl.loop(0, PIECES)
        def _(q):
            mate_term(t, a, layer, q).start()
            if t > 0:
                term(t, a, layer, q).start()
    for a in arrays:
        for copy in states(a):
            copy.start()
    acc[...] = jnp.zeros_like(acc)

    def chip_sum(t, a, layer, q, more, write):
        term(t, a, layer, q).wait()
        mate_term(t, a, layer, q).wait_recv()
        count, at = tiles(a)
        first = mine(targets[t]) * block_rows[a] + q * piece_rows[a]
        second = mates(targets[t]) * block_rows[a] + q * piece_rows[a]

        def tile(i, carry):
            total = new[a][(layer, *at(i, first))].astype(F32) + new[a][(layer, *at(i, second))].astype(F32)
            for ref, index in more:
                total = total + ref[(*index, *at(i, q * piece_rows[a]))].astype(F32)
            return write(i, total, carry)

        return tile, count, at, first

    def summed(t, a, layer, q, more=()):
        def write(i, total, carry):
            new[a][(layer, *at(i, first))] = total.astype(BF16)
            return carry

        tile, count, at, first = chip_sum(t, a, layer, q, more, write)
        lax.fori_loop(0, count, lambda i, carry: tile(i, carry), 0)
        return new[a].at[layer, rows(a, mine(targets[t]), q), :]

    def local(a, q):
        return pl.ds(pl.multiple_of(q * piece_rows[a], piece_rows[a]), piece_rows[a])

    def to_far(way, a, l, q, src):
        return pltpu.make_async_remote_copy(
            src_ref=src, dst_ref=far[a].at[way, l, local(a, q), :],
            send_sem=sum_send.at[way, a], recv_sem=far_sem.at[way, a, l, q], **to(side[way]))

    def to_near(way, a, layer, q, src):
        return pltpu.make_async_remote_copy(
            src_ref=src, dst_ref=near[a].at[way, layer, local(a, q), :],
            send_sem=sum_send.at[way, a], recv_sem=near_sem.at[way, a, layer, q], **to(side[way]))

    for a, l in steps:
        @pl.loop(0, PIECES)
        def _(q):
            for way in WAYS:
                to_far(way, a, l, q, summed(0, a, way * half + l, q)).start()
    for a, l in steps:
        @pl.loop(0, PIECES)
        def _(q):
            for way in WAYS:
                layer = (1 - way) * half + l
                to_near(way, a, layer, q, summed(1 + way, a, layer, q)).start()
    for a, l in steps:
        @pl.loop(0, PIECES)
        def _(q):
            for way in WAYS:
                layer = way * half + l
                src = new[a].at[layer, rows(a, mine(targets[1 + way]), q), :]
                to_far(way, a, l, q, src).wait_recv()
                to_near(way, a, layer, q, summed(1 + way, a, layer, q, [(far[a], (way, l))])).start()
    for a, l in steps:
        @pl.loop(0, PIECES)
        def _(q):
            for layer in (l, half + l):
                for way in WAYS:
                    to_near(way, a, layer, q, near[a].at[way, layer, local(a, q), :]).wait_recv()

                def write(i, total, carry):
                    rounded = total.astype(BF16)
                    near[a][(0, layer, *at(i, q * piece_rows[a]))] = rounded
                    rounded = rounded.astype(F32)
                    square = rounded * rounded
                    for r in range(0, TILE[0], 8):
                        for c in range(0, TILE[1], 128):
                            carry = carry + square[r : r + 8, c : c + 128]
                    return carry

                tile, count, at, _ = chip_sum(3, a, layer, q, [(near[a], (way, layer)) for way in WAYS], write)
                acc[...] = lax.fori_loop(0, count, lambda i, carry: tile(i, carry), acc[...])

    def drain(sem, ref):
        pltpu.make_async_copy(ref, ref, sem).wait()

    squares[me] = acc[...]
    for way in WAYS:
        for a in arrays:
            drain(sum_send.at[way, a], new[a].at[:half, pl.ds(0, 3 * block_rows[a]), :])

    def square(o, device):
        return pltpu.make_async_remote_copy(
            src_ref=squares.at[device], dst_ref=squares.at[device],
            send_sem=square_send.at[o], recv_sem=square_sem.at[device], **to(lax.rem(me + o, n)))

    for o in range(1, n):
        square(o, me).start()
    for a in arrays:
        for copy in states(a):
            copy.wait()
    for o in range(1, n):
        square(o, lax.rem(me + o, n)).wait_recv()
    total = squares[0]
    for i in range(1, n):
        total = total + squares[i]
    total = jnp.sum(jnp.sum(total, axis=1, keepdims=True), axis=0, keepdims=True)
    count = n * sum(ref.size for ref in m)
    factor = jnp.minimum(1.0, 0.5 * lax.rsqrt(total / count + 1e-30))

    def ring(way, a, block, layer, q, sem):
        part = new[a].at[layer, rows(a, block, q), :]
        return pltpu.make_async_remote_copy(
            src_ref=part, dst_ref=part, send_sem=ring_send.at[way, a], recv_sem=sem, **to(side[way]))

    def back(a, block, layer, q):
        part = new[a].at[layer, rows(a, block, q), :]
        return pltpu.make_async_remote_copy(
            src_ref=part, dst_ref=part, send_sem=back_send.at[a], recv_sem=back_sem.at[a], **to(mate))

    for a, l in steps:
        @pl.loop(0, PIECES)
        def _(q):
            tile_count, at = tiles(a)
            for way in WAYS:
                layer = way * half + l

                def tile(i, carry):
                    here = (layer, *at(i, q * piece_rows[a]))
                    gradient = near[a][(0, *here)].astype(F32) * factor
                    mean = 0.9 * m[a][here] + 0.1 * gradient
                    variance = 0.95 * v[a][here] + 0.05 * gradient * gradient
                    weight = own_w[a][here].astype(F32)
                    step = mean * lax.rsqrt(variance + 1e-8) + 0.1 * weight
                    m[a][here] = mean
                    v[a][here] = variance
                    new[a][(layer, *at(i, me * block_rows[a] + q * piece_rows[a]))] = (weight - 0.02 * step).astype(BF16)
                    return carry

                lax.fori_loop(0, tile_count, tile, 0)
                ring(way, a, me, layer, q, ring_sem.at[way, a, layer, q]).start()
                back(a, me, layer, q).start()
    for a, l in steps:
        @pl.loop(0, PIECES)
        def _(q):
            for way in WAYS:
                layer = (1 - way) * half + l
                ring(way, a, me, layer, q, ring_sem.at[way, a, layer, q]).start()
    source = (mine(left_chip), mine(right_chip))
    for a, l in steps:
        @pl.loop(0, PIECES)
        def _(q):
            for way in WAYS:
                layer = way * half + l
                ring(way, a, source[way], layer, q, ring_sem.at[way, a, layer, q]).wait_recv()
                ring(way, a, source[way], layer, q, ringfar_sem.at[way, a, l, q]).start()
                back(a, source[way], layer, q).start()
    for a, l in steps:
        @pl.loop(0, PIECES)
        def _(q):
            for way in WAYS:
                layer = (1 - way) * half + l
                ring(way, a, source[way], layer, q, ring_sem.at[way, a, layer, q]).wait_recv()
                back(a, source[way], layer, q).start()
    for a, l in steps:
        @pl.loop(0, PIECES)
        def _(q):
            for way in WAYS:
                layer = way * half + l
                ring(way, a, mine(far_chip), layer, q, ringfar_sem.at[way, a, l, q]).wait_recv()
                back(a, mine(far_chip), layer, q).start()
    for a in arrays:
        whole = new[a].at[:half]
        drain(back_sem.at[a], whole)
        drain(back_send.at[a], whole)
        drain(mate_send.at[a], whole)
        for way in WAYS:
            drain(ring_send.at[way, a], new[a].at[:half, pl.ds(0, 3 * block_rows[a]), :])
    for o in range(1, n):
        square(o, me).wait_send()


def write_out(*refs):
    count = len(refs) // 2
    copies = [pltpu.make_async_copy(refs[i], refs[count + i], refs[-1].at[i]) for i in range(count)]
    for copy in copies:
        copy.start()
    for copy in copies:
        copy.wait()


def solution(mesh):
    n = mesh.shape["dp"]

    def step(*arrays):
        terms, weights, m, v = (arrays[i : i + 3] for i in (0, 3, 6, 9))
        layers = m[0].shape[0]
        hbm = pl.BlockSpec(memory_space=pltpu.HBM)
        dma = pltpu.SemaphoreType.DMA
        blocks = [one.shape[1:] for one in m]
        out = [(w.shape, BF16) for w in weights] + [(x.shape, F32) for x in (*m, *v)]
        scratch = (
            [pltpu.VMEM((2, layers // 2, *b), BF16) for b in blocks]
            + [pltpu.VMEM((2, layers, *b), BF16) for b in blocks]
            + [pltpu.VMEM((layers, *b), BF16) for b in blocks]
            + [pltpu.VMEM((8, 128), F32), pltpu.VMEM((n, 8, 128), F32)]
            + [dma((4, 3, layers, PIECES)), dma((4, 3, layers, PIECES)), dma((3, 3))]
            + [dma((2, 3, layers // 2, PIECES)), dma((2, 3, layers, PIECES))]
            + [dma((2, 3, layers, PIECES)), dma((2, 3, layers // 2, PIECES))]
            + [dma((3,)), dma((3,)), dma((3,)), dma((2, 3)), dma((2, 3)), dma((n,)), dma((n,))]
        )
        results = pl.pallas_call(
            functools.partial(kernel, n),
            out_shape=[pltpu.VMEM(shape, dtype) for shape, dtype in out],
            in_specs=[hbm] * len(arrays),
            out_specs=[pl.BlockSpec(memory_space=pltpu.VMEM)] * len(out),
            scratch_shapes=scratch,
            compiler_params=pltpu.CompilerParams(
                collective_id=0, has_side_effects=True, vmem_limit_bytes=16 * 2**20),
        )(*arrays)
        return pl.pallas_call(
            write_out,
            out_shape=[jax.ShapeDtypeStruct(shape, dtype) for shape, dtype in out],
            in_specs=[pl.BlockSpec(memory_space=pltpu.VMEM)] * len(out),
            out_specs=[hbm] * len(out),
            scratch_shapes=[dma((len(out),))],
            compiler_params=pltpu.CompilerParams(vmem_limit_bytes=2**20),
        )(*[pltpu.with_memory_space_constraint(x, pltpu.VMEM) for x in results])

    all_of, cut = P(None, None, None), P(None, "dp", None)
    return jax.shard_map(
        step,
        mesh=mesh,
        in_specs=(P(("rep", "dp"), None, None, None),) * 3 + (all_of,) * 3 + (cut,) * 6,
        out_specs=(P("rep", None, None),) * 3 + (P("rep", "dp", None),) * 6,
        check_vma=False,
    )
```

```python
import functools

import jax
import jax.numpy as jnp
from jax import lax
from jax.experimental import pallas as pl
from jax.experimental.pallas import tpu as pltpu
from jax.sharding import PartitionSpec as P

MESH = pl.DeviceIdType.MESH
CORES = 2
PIECES = 4
TILE = (16, 512)
WAYS = (0, 1)
F32, BF16 = jnp.float32, jnp.bfloat16


def kernel(n, *refs):
    g, w, m_in, v_in, new, m, v = (refs[i : i + 3] for i in range(0, 21, 3))
    far, near, own_w = (refs[i : i + 3] for i in range(21, 30, 3))
    (acc, squares, term_sem, mate_sem, state_sem, far_sem, near_sem, ring_sem, ringfar_sem,
     back_sem, mate_send, back_send, sum_send, ring_send, square_send, square_sem) = refs[30:]

    chips = n // CORES
    me = lax.axis_index("dp")
    chip, core = me // CORES, me % CORES
    mate = chip * CORES + 1 - core
    right_chip, left_chip = lax.rem(chip + 1, chips), lax.rem(chip + chips - 1, chips)
    far_chip = lax.rem(chip + 2, chips)
    side = (right_chip * CORES + core, left_chip * CORES + core)
    arrays = range(3)
    layers = m[0].shape[0]
    half = layers // 2
    block_rows = [ref.shape[1] for ref in m]
    piece_rows = [r // PIECES for r in block_rows]
    steps = [(a, l) for l in range(half) for a in arrays]

    def rows(a, block, q):
        return pl.ds(pl.multiple_of(block * block_rows[a] + q * piece_rows[a], piece_rows[a]), piece_rows[a])

    def to(device):
        return {"device_id": {"dp": device}, "device_id_type": MESH}

    def mine(c):
        return c * CORES + core

    def mates(c):
        return c * CORES + 1 - core

    def tiles(a):
        columns = m[a].shape[2] // TILE[1]
        count = piece_rows[a] // TILE[0] * columns

        def at(i, base):
            r = pl.multiple_of(base + i // columns * TILE[0], TILE[0])
            c = pl.multiple_of(i % columns * TILE[1], TILE[1])
            return pl.ds(r, TILE[0]), pl.ds(c, TILE[1])

        return count, at

    targets = (far_chip, right_chip, left_chip, chip)
    places = [(t, a, layer) for t in range(4) for a in arrays for layer in range(layers)]

    def term(t, a, layer, q):
        where = rows(a, mine(targets[t]), q)
        return pltpu.make_async_copy(g[a].at[0, layer, where, :], new[a].at[layer, where, :], term_sem.at[t, a, layer, q])

    def mate_term(t, a, layer, q):
        theirs = new[a].at[layer, rows(a, mine(targets[t]), q), :]
        return pltpu.make_async_remote_copy(
            src_ref=g[a].at[0, layer, rows(a, mates(targets[t]), q), :], dst_ref=theirs,
            send_sem=mate_send.at[a], recv_sem=mate_sem.at[t, a, layer, q], **to(mate))

    def states(a):
        own = pl.ds(pl.multiple_of(me * block_rows[a], block_rows[a]), block_rows[a])
        return (pltpu.make_async_copy(m_in[a], m[a], state_sem.at[0, a]),
                pltpu.make_async_copy(v_in[a], v[a], state_sem.at[1, a]),
                pltpu.make_async_copy(w[a].at[:, own, :], own_w[a], state_sem.at[2, a]))

    barrier = pltpu.get_barrier_semaphore()
    for o in range(1, n):
        pl.semaphore_signal(barrier, inc=1, **to(lax.rem(me + o, n)))
    for t, a, layer in places[: 3 * layers]:
        @pl.loop(0, PIECES)
        def _(q):
            term(t, a, layer, q).start()
    pl.semaphore_wait(barrier, n - 1)

    order = [(t, a, layer) for t in range(4) for a, l in steps for layer in (l, half + l)]
    for t, a, layer in order:
        @pl.loop(0, PIECES)
        def _(q):
            mate_term(t, a, layer, q).start()
            if t > 0:
                term(t, a, layer, q).start()
    for a in arrays:
        for copy in states(a):
            copy.start()
    acc[...] = jnp.zeros_like(acc)

    def chip_sum(t, a, layer, q, more, write):
        term(t, a, layer, q).wait()
        mate_term(t, a, layer, q).wait_recv()
        count, at = tiles(a)
        first = mine(targets[t]) * block_rows[a] + q * piece_rows[a]
        second = mates(targets[t]) * block_rows[a] + q * piece_rows[a]

        def tile(i, carry):
            total = new[a][(layer, *at(i, first))].astype(F32) + new[a][(layer, *at(i, second))].astype(F32)
            for ref, index in more:
                total = total + ref[(*index, *at(i, q * piece_rows[a]))].astype(F32)
            return write(i, total, carry)

        return tile, count, at, first

    def summed(t, a, layer, q, more=()):
        def write(i, total, carry):
            new[a][(layer, *at(i, first))] = total.astype(BF16)
            return carry

        tile, count, at, first = chip_sum(t, a, layer, q, more, write)
        lax.fori_loop(0, count, lambda i, carry: tile(i, carry), 0)
        return new[a].at[layer, rows(a, mine(targets[t]), q), :]

    def local(a, q):
        return pl.ds(pl.multiple_of(q * piece_rows[a], piece_rows[a]), piece_rows[a])

    def to_far(way, a, l, q, src):
        return pltpu.make_async_remote_copy(
            src_ref=src, dst_ref=far[a].at[way, l, local(a, q), :],
            send_sem=sum_send.at[way, a], recv_sem=far_sem.at[way, a, l, q], **to(side[way]))

    def to_near(way, a, layer, q, src):
        return pltpu.make_async_remote_copy(
            src_ref=src, dst_ref=near[a].at[way, layer, local(a, q), :],
            send_sem=sum_send.at[way, a], recv_sem=near_sem.at[way, a, layer, q], **to(side[way]))

    for a, l in steps:
        @pl.loop(0, PIECES)
        def _(q):
            for way in WAYS:
                to_far(way, a, l, q, summed(0, a, way * half + l, q)).start()
    for a, l in steps:
        @pl.loop(0, PIECES)
        def _(q):
            for way in WAYS:
                layer = (1 - way) * half + l
                to_near(way, a, layer, q, summed(1 + way, a, layer, q)).start()
    for a, l in steps:
        @pl.loop(0, PIECES)
        def _(q):
            for way in WAYS:
                layer = way * half + l
                src = new[a].at[layer, rows(a, mine(targets[1 + way]), q), :]
                to_far(way, a, l, q, src).wait_recv()
                to_near(way, a, layer, q, summed(1 + way, a, layer, q, [(far[a], (way, l))])).start()
    for a, l in steps:
        @pl.loop(0, PIECES)
        def _(q):
            for layer in (l, half + l):
                for way in WAYS:
                    to_near(way, a, layer, q, near[a].at[way, layer, local(a, q), :]).wait_recv()

                def write(i, total, carry):
                    rounded = total.astype(BF16)
                    near[a][(0, layer, *at(i, q * piece_rows[a]))] = rounded
                    rounded = rounded.astype(F32)
                    square = rounded * rounded
                    for r in range(0, TILE[0], 8):
                        for c in range(0, TILE[1], 128):
                            carry = carry + square[r : r + 8, c : c + 128]
                    return carry

                tile, count, at, _ = chip_sum(3, a, layer, q, [(near[a], (way, layer)) for way in WAYS], write)
                acc[...] = lax.fori_loop(0, count, lambda i, carry: tile(i, carry), acc[...])

    def drain(sem, ref):
        pltpu.make_async_copy(ref, ref, sem).wait()

    squares[me] = acc[...]
    for way in WAYS:
        for a in arrays:
            drain(sum_send.at[way, a], new[a].at[:half, pl.ds(0, 3 * block_rows[a]), :])

    def square(o, device):
        return pltpu.make_async_remote_copy(
            src_ref=squares.at[device], dst_ref=squares.at[device],
            send_sem=square_send.at[o], recv_sem=square_sem.at[device], **to(lax.rem(me + o, n)))

    for o in range(1, n):
        square(o, me).start()
    for a in arrays:
        for copy in states(a):
            copy.wait()
    for o in range(1, n):
        square(o, lax.rem(me + o, n)).wait_recv()
    total = squares[0]
    for i in range(1, n):
        total = total + squares[i]
    total = jnp.sum(jnp.sum(total, axis=1, keepdims=True), axis=0, keepdims=True)
    count = n * sum(ref.size for ref in m)
    factor = jnp.minimum(1.0, 0.5 * lax.rsqrt(total / count + 1e-30))

    def ring(way, a, block, layer, q, sem):
        part = new[a].at[layer, rows(a, block, q), :]
        return pltpu.make_async_remote_copy(
            src_ref=part, dst_ref=part, send_sem=ring_send.at[way, a], recv_sem=sem, **to(side[way]))

    def back(a, block, layer, q):
        part = new[a].at[layer, rows(a, block, q), :]
        return pltpu.make_async_remote_copy(
            src_ref=part, dst_ref=part, send_sem=back_send.at[a], recv_sem=back_sem.at[a], **to(mate))

    for a, l in steps:
        @pl.loop(0, PIECES)
        def _(q):
            tile_count, at = tiles(a)
            for way in WAYS:
                layer = way * half + l

                def tile(i, carry):
                    here = (layer, *at(i, q * piece_rows[a]))
                    gradient = near[a][(0, *here)].astype(F32) * factor
                    mean = 0.9 * m[a][here] + 0.1 * gradient
                    variance = 0.95 * v[a][here] + 0.05 * gradient * gradient
                    weight = own_w[a][here].astype(F32)
                    step = mean * lax.rsqrt(variance + 1e-8) + 0.1 * weight
                    m[a][here] = mean
                    v[a][here] = variance
                    new[a][(layer, *at(i, me * block_rows[a] + q * piece_rows[a]))] = (weight - 0.02 * step).astype(BF16)
                    return carry

                lax.fori_loop(0, tile_count, tile, 0)
                ring(way, a, me, layer, q, ring_sem.at[way, a, layer, q]).start()
                back(a, me, layer, q).start()
    for a, l in steps:
        @pl.loop(0, PIECES)
        def _(q):
            for way in WAYS:
                layer = (1 - way) * half + l
                ring(way, a, me, layer, q, ring_sem.at[way, a, layer, q]).start()
    source = (mine(left_chip), mine(right_chip))
    for a, l in steps:
        @pl.loop(0, PIECES)
        def _(q):
            for way in WAYS:
                layer = way * half + l
                ring(way, a, source[way], layer, q, ring_sem.at[way, a, layer, q]).wait_recv()
                ring(way, a, source[way], layer, q, ringfar_sem.at[way, a, l, q]).start()
                back(a, source[way], layer, q).start()
    for a, l in steps:
        @pl.loop(0, PIECES)
        def _(q):
            for way in WAYS:
                layer = (1 - way) * half + l
                ring(way, a, source[way], layer, q, ring_sem.at[way, a, layer, q]).wait_recv()
                back(a, source[way], layer, q).start()
    for a, l in steps:
        @pl.loop(0, PIECES)
        def _(q):
            for way in WAYS:
                layer = way * half + l
                ring(way, a, mine(far_chip), layer, q, ringfar_sem.at[way, a, l, q]).wait_recv()
                back(a, mine(far_chip), layer, q).start()
    for a in arrays:
        whole = new[a].at[:half]
        drain(back_sem.at[a], whole)
        drain(back_send.at[a], whole)
        drain(mate_send.at[a], whole)
        for way in WAYS:
            drain(ring_send.at[way, a], new[a].at[:half, pl.ds(0, 3 * block_rows[a]), :])
    for o in range(1, n):
        square(o, me).wait_send()


def write_out(*refs):
    count = len(refs) // 2
    copies = [pltpu.make_async_copy(refs[i], refs[count + i], refs[-1].at[i]) for i in range(count)]
    for copy in copies:
        copy.start()
    for copy in copies:
        copy.wait()


def solution(mesh):
    n = mesh.shape["dp"]

    def step(*arrays):
        terms, weights, m, v = (arrays[i : i + 3] for i in (0, 3, 6, 9))
        layers = m[0].shape[0]
        hbm = pl.BlockSpec(memory_space=pltpu.HBM)
        dma = pltpu.SemaphoreType.DMA
        blocks = [one.shape[1:] for one in m]
        out = [(w.shape, BF16) for w in weights] + [(x.shape, F32) for x in (*m, *v)]
        scratch = (
            [pltpu.VMEM((2, layers // 2, *b), BF16) for b in blocks]
            + [pltpu.VMEM((2, layers, *b), BF16) for b in blocks]
            + [pltpu.VMEM((layers, *b), BF16) for b in blocks]
            + [pltpu.VMEM((8, 128), F32), pltpu.VMEM((n, 8, 128), F32)]
            + [dma((4, 3, layers, PIECES)), dma((4, 3, layers, PIECES)), dma((3, 3))]
            + [dma((2, 3, layers // 2, PIECES)), dma((2, 3, layers, PIECES))]
            + [dma((2, 3, layers, PIECES)), dma((2, 3, layers // 2, PIECES))]
            + [dma((3,)), dma((3,)), dma((3,)), dma((2, 3)), dma((2, 3)), dma((n,)), dma((n,))]
        )
        results = pl.pallas_call(
            functools.partial(kernel, n),
            out_shape=[pltpu.VMEM(shape, dtype) for shape, dtype in out],
            in_specs=[hbm] * len(arrays),
            out_specs=[pl.BlockSpec(memory_space=pltpu.VMEM)] * len(out),
            scratch_shapes=scratch,
            compiler_params=pltpu.CompilerParams(
                collective_id=0, has_side_effects=True, vmem_limit_bytes=16 * 2**20),
        )(*arrays)
        return pl.pallas_call(
            write_out,
            out_shape=[jax.ShapeDtypeStruct(shape, dtype) for shape, dtype in out],
            in_specs=[pl.BlockSpec(memory_space=pltpu.VMEM)] * len(out),
            out_specs=[hbm] * len(out),
            scratch_shapes=[dma((len(out),))],
            compiler_params=pltpu.CompilerParams(vmem_limit_bytes=16 * 2**20),
        )(*[pltpu.with_memory_space_constraint(x, pltpu.VMEM) for x in results])

    all_of, cut = P(None, None, None), P(None, "dp", None)
    return jax.shard_map(
        step,
        mesh=mesh,
        in_specs=(P(("rep", "dp"), None, None, None),) * 3 + (all_of,) * 3 + (cut,) * 6,
        out_specs=(P("rep", None, None),) * 3 + (P("rep", "dp", None),) * 6,
        check_vma=False,
    )
```

```python
import functools

import jax
import jax.numpy as jnp
from jax import lax
from jax.experimental import pallas as pl
from jax.experimental.pallas import tpu as pltpu
from jax.sharding import PartitionSpec as P

MESH = pl.DeviceIdType.MESH
CORES = 2
PIECES = 8
TILE = (16, 512)
WAYS = (0, 1)
F32, BF16 = jnp.float32, jnp.bfloat16


def kernel(n, fine, *refs):
    g, w, m_in, v_in, new, m, v = (refs[i : i + 3] for i in range(0, 21, 3))
    far, near, own_w = (refs[i : i + 3] for i in range(21, 30, 3))
    (stage, acc, squares, term_sem, mate_sem, head_sem, stage_sem, state_sem, first_sem, second_sem, last_sem,
     back_sem, mate_send, back_send, sum_send, ring_send, square_sem) = refs[30:]

    chips = n // CORES
    me = lax.axis_index("dp")
    chip, core = me // CORES, me % CORES
    mate = chip * CORES + 1 - core
    right_chip, left_chip = lax.rem(chip + 1, chips), lax.rem(chip + chips - 1, chips)
    far_chip = lax.rem(chip + 2, chips)
    side = (right_chip * CORES + core, left_chip * CORES + core)
    layers = m[0].shape[0]
    half = layers // 2
    height = [ref.shape[1] for ref in m]
    arrays = [a for a in range(3) if a != fine] + [fine]
    steps = [(k, a, l) for k, (l, a) in enumerate((l, a) for l in range(half) for a in arrays)]
    final = len(steps) - 1
    head_first = steps[final:] + steps[:final]

    def to(device):
        return {"device_id": {"dp": device}, "device_id_type": MESH}

    def mine(c):
        return c * CORES + core

    def mates(c):
        return c * CORES + 1 - core

    def block(a, index, start=0, size=None):
        size = size or height[a]
        return pl.ds(pl.multiple_of(index * height[a] + start, size), size)

    def pieces(k, a, body):
        if k < final:
            body(0, 0, height[a])
        else:
            size = height[a] // PIECES
            pl.loop(0, PIECES)(lambda q: body(q, q * size, size))

    def tiles(a, size, body, carry):
        columns = m[a].shape[2] // TILE[1]

        def tile(i, carry):
            def at(base):
                r = pl.multiple_of(base + i // columns * TILE[0], TILE[0])
                return pl.ds(r, TILE[0]), pl.ds(pl.multiple_of(i % columns * TILE[1], TILE[1]), TILE[1])

            return body(at, carry)

        return lax.fori_loop(0, size // TILE[0] * columns, tile, carry)

    def drain(sem, ref):
        pltpu.make_async_copy(ref, ref, sem).wait()

    targets = (far_chip, right_chip, left_chip, chip)

    def term(t, a):
        where = block(a, mine(targets[t]))
        return pltpu.make_async_copy(g[a].at[0, :, where, :], new[a].at[:, where, :], term_sem.at[t, a])

    def mate_term(t, a):
        return pltpu.make_async_remote_copy(
            src_ref=g[a].at[0, :, block(a, mates(targets[t])), :], dst_ref=new[a].at[:, block(a, mine(targets[t])), :],
            send_sem=mate_send.at[a], recv_sem=mate_sem.at[t, a], **to(mate))

    def mate_head(q):
        size = height[fine] // PIECES
        return pltpu.make_async_remote_copy(
            src_ref=stage.at[:, block(fine, 0, q * size, size), :],
            dst_ref=new[fine].at[:, block(fine, mine(far_chip), q * size, size), :],
            send_sem=mate_send.at[fine], recv_sem=head_sem.at[q], **to(mate))

    to_stage = pltpu.make_async_copy(g[fine].at[0, :, block(fine, mates(far_chip)), :], stage, stage_sem.at[0])

    def states(a):
        return (pltpu.make_async_copy(m_in[a], m[a], state_sem.at[0, a]),
                pltpu.make_async_copy(v_in[a], v[a], state_sem.at[1, a]),
                pltpu.make_async_copy(w[a].at[:, block(a, me), :], own_w[a], state_sem.at[2, a]))

    barrier = pltpu.get_barrier_semaphore()
    for o in range(1, n):
        pl.semaphore_signal(barrier, inc=1, **to(lax.rem(me + o, n)))
    to_stage.start()
    for a in (fine, *arrays[:-1]):
        term(0, a).start()
    to_stage.wait()
    pl.semaphore_wait(barrier, n - 1)
    pl.loop(0, PIECES)(lambda q: mate_head(q).start())
    for t, a in [(0, a) for a in arrays[:-1]] + [(t, a) for a in arrays for t in (1, 2)] + [(3, a) for a in arrays]:
        mate_term(t, a).start()
        if t > 0:
            term(t, a).start()
    for a in arrays:
        for copy in states(a):
            copy.start()
    acc[...] = jnp.zeros_like(acc)

    arrived = set()

    def await_terms(t, a):
        if (t, a) not in arrived:
            arrived.add((t, a))
            term(t, a).wait()
            if (t, a) == (0, fine):
                return lambda q: mate_head(q).wait_recv()
            mate_term(t, a).wait_recv()
        return lambda q: None

    def total(t, a, layer, at, start, more):
        out = new[a][(layer, *at(mine(targets[t]) * height[a] + start))].astype(F32)
        out = out + new[a][(layer, *at(mates(targets[t]) * height[a] + start))].astype(F32)
        for ref, index in more:
            out = out + ref[(*index, *at(start))].astype(F32)
        return out

    def summed(t, a, layer, start, size, more=()):
        def tile(at, carry):
            new[a][(layer, *at(mine(targets[t]) * height[a] + start))] = total(t, a, layer, at, start, more).astype(BF16)
            return carry

        tiles(a, size, tile, 0)
        return new[a].at[layer, block(a, mine(targets[t]), start, size), :]

    def send_sum(way, a, src, dst, sem):
        pltpu.make_async_remote_copy(
            src_ref=src, dst_ref=dst, send_sem=sum_send.at[way, a], recv_sem=sem, **to(side[way])).start()

    def part(a, start, size):
        return pl.ds(pl.multiple_of(start, size), size)

    for k, a, l in head_first:
        here = await_terms(0, a)

        def body(q, start, size):
            here(q)
            for way in WAYS:
                src = summed(0, a, way * half + l, start, size)
                send_sum(way, a, src, far[a].at[way, l, part(a, start, size), :], first_sem.at[way, k])

        pieces(k, a, body)
    for k, a, l in steps:
        for way in WAYS:
            await_terms(1 + way, a)
            layer = (1 - way) * half + l
            src = summed(1 + way, a, layer, 0, height[a])
            send_sum(way, a, src, near[a].at[way, layer], second_sem.at[way, k])
    for k, a, l in steps:
        for way in WAYS:
            drain(first_sem.at[way, k], far[a].at[way, l])

        def body(q, start, size):
            for way in WAYS:
                layer = way * half + l
                src = summed(1 + way, a, layer, start, size, [(far[a], (way, l))])
                send_sum(way, a, src, near[a].at[way, layer, part(a, start, size), :], last_sem.at[way, k + q])

        pieces(k, a, body)
    for k, a, l in steps:
        await_terms(3, a)
        for way in WAYS:
            drain(second_sem.at[way, k], near[a].at[way, (1 - way) * half + l])

        def body(q, start, size):
            for way in WAYS:
                layer = way * half + l
                drain(last_sem.at[way, k + q], near[a].at[way, layer, part(a, start, size), :])

                def tile(at, carry):
                    rounded = total(3, a, layer, at, start, [(near[a], (i, layer)) for i in WAYS]).astype(BF16)
                    near[a][(0, layer, *at(start))] = rounded
                    rounded = rounded.astype(F32)
                    square = rounded * rounded
                    for r in range(0, TILE[0], 8):
                        for c in range(0, TILE[1], 128):
                            carry = carry + square[r : r + 8, c : c + 128]
                    return carry

                acc[...] = tiles(a, size, tile, acc[...])

        pieces(k, a, body)

    squares[me] = acc[...]
    for way in WAYS:
        for a in arrays:
            drain(sum_send.at[way, a], new[a].at[:half, pl.ds(0, 3 * height[a]), :])
    for o in range(1, n):
        pltpu.make_async_remote_copy(
            src_ref=squares.at[me], dst_ref=squares.at[me], send_sem=square_sem.at[0], recv_sem=square_sem.at[1],
            **to(lax.rem(me + o, n))).start()
    for a in arrays:
        for copy in states(a):
            copy.wait()
    drain(square_sem.at[1], squares.at[pl.ds(0, n - 1)])
    everyone = squares[0]
    for i in range(1, n):
        everyone = everyone + squares[i]
    everyone = jnp.sum(jnp.sum(everyone, axis=1, keepdims=True), axis=0, keepdims=True)
    count = n * sum(ref.size for ref in m)
    factor = jnp.minimum(1.0, 0.5 * lax.rsqrt(everyone / count + 1e-30))

    def ring(way, a, index, layer, start, size, sem):
        here = new[a].at[layer, block(a, index, start, size), :]
        pltpu.make_async_remote_copy(
            src_ref=here, dst_ref=here, send_sem=ring_send.at[way, a], recv_sem=sem, **to(side[way])).start()

    def back(a, index, layer, start, size):
        here = new[a].at[layer, block(a, index, start, size), :]
        pltpu.make_async_remote_copy(
            src_ref=here, dst_ref=here, send_sem=back_send.at[a], recv_sem=back_sem.at[a], **to(mate)).start()

    for k, a, l in head_first:
        def body(q, start, size):
            for way in WAYS:
                layer = way * half + l

                def tile(at, carry):
                    here = (layer, *at(start))
                    gradient = near[a][(0, *here)].astype(F32) * factor
                    mean = 0.9 * m[a][here] + 0.1 * gradient
                    variance = 0.95 * v[a][here] + 0.05 * gradient * gradient
                    weight = own_w[a][here].astype(F32)
                    step = mean * lax.rsqrt(variance + 1e-8) + 0.1 * weight
                    m[a][here] = mean
                    v[a][here] = variance
                    new[a][(layer, *at(me * height[a] + start))] = (weight - 0.02 * step).astype(BF16)
                    return carry

                tiles(a, size, tile, 0)
                ring(way, a, me, layer, start, size, first_sem.at[way, k])
                back(a, me, layer, start, size)

        pieces(k, a, body)
    for k, a, l in steps:
        for way in WAYS:
            ring(way, a, me, (1 - way) * half + l, 0, height[a], second_sem.at[way, k])
    source = (mine(left_chip), mine(right_chip))
    for k, a, l in head_first:
        for way in WAYS:
            layer = way * half + l
            drain(first_sem.at[way, k], new[a].at[layer, block(a, source[way]), :])
            back(a, source[way], layer, 0, height[a])
    for k, a, l in steps:
        def body(q, start, size):
            for way in WAYS:
                ring(way, a, source[way], way * half + l, start, size, last_sem.at[way, k + q])

        pieces(k, a, body)
    for k, a, l in steps:
        for way in WAYS:
            layer = (1 - way) * half + l
            drain(second_sem.at[way, k], new[a].at[layer, block(a, source[way]), :])
            back(a, source[way], layer, 0, height[a])
    for k, a, l in steps:
        def body(q, start, size):
            for way in WAYS:
                layer = way * half + l
                drain(last_sem.at[way, k + q], new[a].at[layer, block(a, mine(far_chip), start, size), :])
                back(a, mine(far_chip), layer, start, size)

        pieces(k, a, body)
    for a in arrays:
        for sem in (mate_send, back_send, back_sem):
            drain(sem.at[a], new[a].at[:half])
        for way in WAYS:
            drain(ring_send.at[way, a], new[a].at[:half, pl.ds(0, 3 * height[a]), :])
    drain(square_sem.at[0], squares.at[pl.ds(0, n - 1)])


def write_out(*refs):
    count = len(refs) // 2
    copies = [pltpu.make_async_copy(refs[i], refs[count + i], refs[-1].at[i]) for i in range(count)]
    for copy in copies:
        copy.start()
    for copy in copies:
        copy.wait()


def solution(mesh):
    n = mesh.shape["dp"]

    def step(*arrays):
        terms, weights, m, v = (arrays[i : i + 3] for i in (0, 3, 6, 9))
        layers = m[0].shape[0]
        hbm = pl.BlockSpec(memory_space=pltpu.HBM)
        dma = pltpu.SemaphoreType.DMA
        blocks = [one.shape[1:] for one in m]
        out = [(w.shape, BF16) for w in weights] + [(x.shape, F32) for x in (*m, *v)]
        fine = max(range(3), key=lambda a: blocks[a][0])
        steps = 3 * (layers // 2)
        scratch = (
            [pltpu.VMEM((2, layers // 2, *b), BF16) for b in blocks]
            + [pltpu.VMEM((2, layers, *b), BF16) for b in blocks]
            + [pltpu.VMEM((layers, *b), BF16) for b in blocks]
            + [pltpu.VMEM((layers, *blocks[fine]), BF16), pltpu.VMEM((8, 128), F32), pltpu.VMEM((n, 8, 128), F32)]
            + [dma((4, 3)), dma((4, 3)), dma((PIECES,)), dma((1,)), dma((3, 3))]
            + [dma((2, steps)), dma((2, steps)), dma((2, steps - 1 + PIECES))]
            + [dma((3,)), dma((3,)), dma((3,)), dma((2, 3)), dma((2, 3)), dma((2,))]
        )
        results = pl.pallas_call(
            functools.partial(kernel, n, fine),
            out_shape=[pltpu.VMEM(shape, dtype) for shape, dtype in out],
            in_specs=[hbm] * len(arrays),
            out_specs=[pl.BlockSpec(memory_space=pltpu.VMEM)] * len(out),
            scratch_shapes=scratch,
            compiler_params=pltpu.CompilerParams(
                collective_id=0, has_side_effects=True, vmem_limit_bytes=16 * 2**20),
        )(*arrays)
        return pl.pallas_call(
            write_out,
            out_shape=[jax.ShapeDtypeStruct(shape, dtype) for shape, dtype in out],
            in_specs=[pl.BlockSpec(memory_space=pltpu.VMEM)] * len(out),
            out_specs=[hbm] * len(out),
            scratch_shapes=[dma((len(out),))],
            compiler_params=pltpu.CompilerParams(vmem_limit_bytes=16 * 2**20),
        )(*[pltpu.with_memory_space_constraint(x, pltpu.VMEM) for x in results])

    all_of, cut = P(None, None, None), P(None, "dp", None)
    return jax.shard_map(
        step,
        mesh=mesh,
        in_specs=(P(("rep", "dp"), None, None, None),) * 3 + (all_of,) * 3 + (cut,) * 6,
        out_specs=(P("rep", None, None),) * 3 + (P("rep", "dp", None),) * 6,
        check_vma=False,
    )
```

```python
import functools

import jax
import jax.numpy as jnp
from jax import lax
from jax.experimental import pallas as pl
from jax.experimental.pallas import tpu as pltpu
from jax.sharding import PartitionSpec as P

MESH = pl.DeviceIdType.MESH
CORES = 2
PIECES = 8
LAST_PIECES = 4
TILE = (16, 512)
WAYS = (0, 1)
F32, BF16 = jnp.float32, jnp.bfloat16
VMEM_LIMIT = 16 * 2**20


def kernel(n, fine, *refs):
    g, w, m_in, v_in, new, m, v = (refs[i : i + 3] for i in range(0, 21, 3))
    tail, *refs = refs[21:]
    far, near, own_w = (refs[i : i + 3] for i in range(0, 9, 3))
    (stage, acc, squares, term_sem, mate_sem, head_sem, stage_sem, state_sem, first_sem, second_sem, last_sem,
     back_sem, mate_send, back_send, sum_send, ring_send, square_sem, tail_sem) = refs[9:]

    chips = n // CORES
    me = lax.axis_index("dp")
    chip, core = me // CORES, me % CORES
    mate = chip * CORES + 1 - core
    right_chip, left_chip = lax.rem(chip + 1, chips), lax.rem(chip + chips - 1, chips)
    far_chip = lax.rem(chip + 2, chips)
    side = (right_chip * CORES + core, left_chip * CORES + core)
    layers = m[0].shape[0]
    half = layers // 2
    height = [ref.shape[1] for ref in m]
    arrays = [a for a in range(3) if a != fine] + [fine]
    steps = [(k, a, l) for k, (l, a) in enumerate((l, a) for l in range(half) for a in arrays)]
    final = len(steps) - 1
    head_first = steps[final:] + steps[:final]

    def to(device):
        return {"device_id": {"dp": device}, "device_id_type": MESH}

    def mine(c):
        return c * CORES + core

    def mates(c):
        return c * CORES + 1 - core

    def block(a, index, start=0, size=None):
        size = size or height[a]
        return pl.ds(pl.multiple_of(index * height[a] + start, size), size)

    def pieces(k, a, body):
        if k < final:
            body(0, 0, height[a])
        else:
            size = height[a] // PIECES
            pl.loop(0, PIECES)(lambda q: body(q, q * size, size))

    def tiles(a, size, body, carry):
        columns = m[a].shape[2] // TILE[1]

        def tile(i, carry):
            def at(base):
                r = pl.multiple_of(base + i // columns * TILE[0], TILE[0])
                return pl.ds(r, TILE[0]), pl.ds(pl.multiple_of(i % columns * TILE[1], TILE[1]), TILE[1])

            return body(at, carry)

        return lax.fori_loop(0, size // TILE[0] * columns, tile, carry)

    def drain(sem, ref):
        pltpu.make_async_copy(ref, ref, sem).wait()

    targets = (far_chip, right_chip, left_chip, chip)

    def term(t, a):
        where = block(a, mine(targets[t]))
        return pltpu.make_async_copy(g[a].at[0, :, where, :], new[a].at[:, where, :], term_sem.at[t, a])

    def mate_term(t, a):
        return pltpu.make_async_remote_copy(
            src_ref=g[a].at[0, :, block(a, mates(targets[t])), :], dst_ref=new[a].at[:, block(a, mine(targets[t])), :],
            send_sem=mate_send.at[a], recv_sem=mate_sem.at[t, a], **to(mate))

    def mate_head(q):
        size = height[fine] // PIECES
        return pltpu.make_async_remote_copy(
            src_ref=stage.at[:, block(fine, 0, q * size, size), :],
            dst_ref=new[fine].at[:, block(fine, mine(far_chip), q * size, size), :],
            send_sem=mate_send.at[fine], recv_sem=head_sem.at[q], **to(mate))

    to_stage = pltpu.make_async_copy(g[fine].at[0, :, block(fine, mates(far_chip)), :], stage, stage_sem.at[0])

    def states(a):
        return (pltpu.make_async_copy(m_in[a], m[a], state_sem.at[0, a]),
                pltpu.make_async_copy(v_in[a], v[a], state_sem.at[1, a]),
                pltpu.make_async_copy(w[a].at[:, block(a, me), :], own_w[a], state_sem.at[2, a]))

    barrier = pltpu.get_barrier_semaphore()
    for o in range(1, n):
        pl.semaphore_signal(barrier, inc=1, **to(lax.rem(me + o, n)))
    to_stage.start()
    for a in (fine, *arrays[:-1]):
        term(0, a).start()
    to_stage.wait()
    pl.semaphore_wait(barrier, n - 1)
    pl.loop(0, PIECES)(lambda q: mate_head(q).start())
    for t, a in [(0, a) for a in arrays[:-1]] + [(t, a) for a in arrays for t in (1, 2)] + [(3, a) for a in arrays]:
        mate_term(t, a).start()
        if t > 0:
            term(t, a).start()
    for a in arrays:
        for copy in states(a):
            copy.start()
    acc[...] = jnp.zeros_like(acc)

    arrived = set()

    def await_terms(t, a):
        if (t, a) not in arrived:
            arrived.add((t, a))
            term(t, a).wait()
            if (t, a) == (0, fine):
                return lambda q: mate_head(q).wait_recv()
            mate_term(t, a).wait_recv()
        return lambda q: None

    def total(t, a, layer, at, start, more):
        out = new[a][(layer, *at(mine(targets[t]) * height[a] + start))].astype(F32)
        out = out + new[a][(layer, *at(mates(targets[t]) * height[a] + start))].astype(F32)
        for ref, index in more:
            out = out + ref[(*index, *at(start))].astype(F32)
        return out

    def summed(t, a, layer, start, size, more=()):
        def tile(at, carry):
            new[a][(layer, *at(mine(targets[t]) * height[a] + start))] = total(t, a, layer, at, start, more).astype(BF16)
            return carry

        tiles(a, size, tile, 0)
        return new[a].at[layer, block(a, mine(targets[t]), start, size), :]

    def send_sum(way, a, src, dst, sem):
        pltpu.make_async_remote_copy(
            src_ref=src, dst_ref=dst, send_sem=sum_send.at[way, a], recv_sem=sem, **to(side[way])).start()

    def part(a, start, size):
        return pl.ds(pl.multiple_of(start, size), size)

    for k, a, l in head_first:
        here = await_terms(0, a)

        def body(q, start, size):
            here(q)
            for way in WAYS:
                src = summed(0, a, way * half + l, start, size)
                send_sum(way, a, src, far[a].at[way, l, part(a, start, size), :], first_sem.at[way, k])

        pieces(k, a, body)
    for k, a, l in steps:
        for way in WAYS:
            await_terms(1 + way, a)
            layer = (1 - way) * half + l
            src = summed(1 + way, a, layer, 0, height[a])
            send_sum(way, a, src, near[a].at[way, layer], second_sem.at[way, k])
    for k, a, l in steps:
        for way in WAYS:
            drain(first_sem.at[way, k], far[a].at[way, l])

        def body(q, start, size):
            for way in WAYS:
                layer = way * half + l
                src = summed(1 + way, a, layer, start, size, [(far[a], (way, l))])
                send_sum(way, a, src, near[a].at[way, layer, part(a, start, size), :], last_sem.at[way, k + q])

        pieces(k, a, body)
    for k, a, l in steps:
        await_terms(3, a)
        for way in WAYS:
            drain(second_sem.at[way, k], near[a].at[way, (1 - way) * half + l])

        def body(q, start, size):
            for way in WAYS:
                layer = way * half + l
                drain(last_sem.at[way, k + q], near[a].at[way, layer, part(a, start, size), :])

                def tile(at, carry):
                    rounded = total(3, a, layer, at, start, [(near[a], (i, layer)) for i in WAYS]).astype(BF16)
                    near[a][(0, layer, *at(start))] = rounded
                    rounded = rounded.astype(F32)
                    square = rounded * rounded
                    for r in range(0, TILE[0], 8):
                        for c in range(0, TILE[1], 128):
                            carry = carry + square[r : r + 8, c : c + 128]
                    return carry

                acc[...] = tiles(a, size, tile, acc[...])

        pieces(k, a, body)

    squares[me] = acc[...]
    for way in WAYS:
        for a in arrays:
            drain(sum_send.at[way, a], new[a].at[:half, pl.ds(0, 3 * height[a]), :])
    for o in range(1, n):
        pltpu.make_async_remote_copy(
            src_ref=squares.at[me], dst_ref=squares.at[me], send_sem=square_sem.at[0], recv_sem=square_sem.at[1],
            **to(lax.rem(me + o, n))).start()
    for a in arrays:
        for copy in states(a):
            copy.wait()
    drain(square_sem.at[1], squares.at[pl.ds(0, n - 1)])
    everyone = squares[0]
    for i in range(1, n):
        everyone = everyone + squares[i]
    everyone = jnp.sum(jnp.sum(everyone, axis=1, keepdims=True), axis=0, keepdims=True)
    count = n * sum(ref.size for ref in m)
    factor = jnp.minimum(1.0, 0.5 * lax.rsqrt(everyone / count + 1e-30))

    def ring(way, a, index, layer, start, size, sem):
        here = new[a].at[layer, block(a, index, start, size), :]
        pltpu.make_async_remote_copy(
            src_ref=here, dst_ref=here, send_sem=ring_send.at[way, a], recv_sem=sem, **to(side[way])).start()

    def back(a, index, layer, start, size):
        here = new[a].at[layer, block(a, index, start, size), :]
        pltpu.make_async_remote_copy(
            src_ref=here, dst_ref=here, send_sem=back_send.at[a], recv_sem=back_sem.at[a], **to(mate)).start()

    for k, a, l in head_first:
        def body(q, start, size):
            for way in WAYS:
                layer = way * half + l

                def tile(at, carry):
                    here = (layer, *at(start))
                    gradient = near[a][(0, *here)].astype(F32) * factor
                    mean = 0.9 * m[a][here] + 0.1 * gradient
                    variance = 0.95 * v[a][here] + 0.05 * gradient * gradient
                    weight = own_w[a][here].astype(F32)
                    step = mean * lax.rsqrt(variance + 1e-8) + 0.1 * weight
                    m[a][here] = mean
                    v[a][here] = variance
                    new[a][(layer, *at(me * height[a] + start))] = (weight - 0.02 * step).astype(BF16)
                    return carry

                tiles(a, size, tile, 0)
                ring(way, a, me, layer, start, size, first_sem.at[way, k])
                back(a, me, layer, start, size)

        pieces(k, a, body)
    for k, a, l in steps:
        for way in WAYS:
            ring(way, a, me, (1 - way) * half + l, 0, height[a], second_sem.at[way, k])
    source = (mine(left_chip), mine(right_chip))
    for k, a, l in head_first:
        for way in WAYS:
            layer = way * half + l
            drain(first_sem.at[way, k], new[a].at[layer, block(a, source[way]), :])
            if k < final:
                back(a, source[way], layer, 0, height[a])
            else:
                here = new[a].at[layer, block(a, source[way]), :]
                pltpu.make_async_remote_copy(
                    src_ref=here, dst_ref=here, send_sem=tail_sem.at[2], recv_sem=tail_sem.at[way], **to(mate)).start()

    def last_pieces(k, a, body):
        if k < final - 1:
            body(0, 0, height[a])
        else:
            size = height[a] // LAST_PIECES
            pl.loop(0, LAST_PIECES)(lambda q: body(q, q * size, size))

    for k, a, l in steps[:final]:
        def body(q, start, size):
            for way in WAYS:
                ring(way, a, source[way], way * half + l, start, size, last_sem.at[way, k + q])

        last_pieces(k, a, body)
    for k, a, l in steps:
        for way in WAYS:
            layer = (1 - way) * half + l
            drain(second_sem.at[way, k], new[a].at[layer, block(a, source[way]), :])
            back(a, source[way], layer, 0, height[a])
    _, a, l = steps[final]
    for way in WAYS:
        drain(tail_sem.at[way], new[a].at[way * half + l, block(a, mates((left_chip, right_chip)[way])), :])
    pair = CORES * height[a]
    where = pl.ds(pl.multiple_of((left_chip + core * (right_chip - left_chip)) * pair, pair), pair)
    to_tail = pltpu.make_async_copy(new[a].at[core * half + l, where, :], tail, tail_sem.at[3])
    to_tail.start()
    for k, a, l in steps[:final]:
        def body(q, start, size):
            for way in WAYS:
                layer = way * half + l
                drain(last_sem.at[way, k + q], new[a].at[layer, block(a, mine(far_chip), start, size), :])
                back(a, mine(far_chip), layer, start, size)

        last_pieces(k, a, body)
    to_tail.wait()
    drain(tail_sem.at[2], new[fine].at[0, pl.ds(0, 2 * height[fine]), :])
    for a in arrays:
        drain(mate_send.at[a], new[a].at[:half])
        for sem in (back_send, back_sem):
            drain(sem.at[a], new[a].at[:half] if a != fine else new[a].at[: layers - 1, pl.ds(0, 4 * height[a]), :])
        for way in WAYS:
            blocks = 3 * half - (a == fine)
            drain(ring_send.at[way, a], new[a].at[0, pl.ds(0, blocks * height[a]), :])
    drain(square_sem.at[0], squares.at[pl.ds(0, n - 1)])


def solution(mesh):
    n = mesh.shape["dp"]
    chips = n // CORES
    onward = [(i, (i // CORES + (1 if i % CORES == 0 else chips - 1)) % chips * CORES + i % CORES) for i in range(n)]
    mates = [(i, i // CORES * CORES + 1 - i % CORES) for i in range(n)]

    def step(*arrays):
        terms, weights, m, v = (arrays[i : i + 3] for i in (0, 3, 6, 9))
        layers = m[0].shape[0]
        hbm = pl.BlockSpec(memory_space=pltpu.HBM)
        vmem = pl.BlockSpec(memory_space=pltpu.VMEM)
        dma = pltpu.SemaphoreType.DMA
        blocks = [one.shape[1:] for one in m]
        fine = max(range(3), key=lambda a: blocks[a][0])
        out = [(w.shape, BF16) for w in weights] + [(x.shape, F32) for x in (*m, *v)]
        steps = 3 * (layers // 2)
        rows, columns = blocks[fine]
        scratch = (
            [pltpu.VMEM((2, layers // 2, *b), BF16) for b in blocks]
            + [pltpu.VMEM((2, layers, *b), BF16) for b in blocks]
            + [pltpu.VMEM((layers, *b), BF16) for b in blocks]
            + [pltpu.VMEM((layers, *blocks[fine]), BF16), pltpu.VMEM((8, 128), F32), pltpu.VMEM((n, 8, 128), F32)]
            + [dma((4, 3)), dma((4, 3)), dma((PIECES,)), dma((1,)), dma((3, 3))]
            + [dma((2, steps)), dma((2, steps)), dma((2, steps - 1 + PIECES))]
            + [dma((3,)), dma((3,)), dma((3,)), dma((2, 3)), dma((2, 3)), dma((2,)), dma((4,))]
        )
        *results, tail = pl.pallas_call(
            functools.partial(kernel, n, fine),
            out_shape=[pltpu.VMEM(shape, dtype) for shape, dtype in [*out, ((CORES * rows, columns), BF16)]],
            in_specs=[hbm] * len(arrays),
            out_specs=[vmem] * (len(out) + 1),
            scratch_shapes=scratch,
            compiler_params=pltpu.CompilerParams(
                collective_id=0, has_side_effects=True, vmem_limit_bytes=VMEM_LIMIT),
        )(*arrays)

        def held(x):
            return pltpu.with_memory_space_constraint(x, pltpu.VMEM)

        def write(indices, place=None, part=None, whole=None):
            sources = [held(results[i]) for i in indices]
            shapes = [jax.ShapeDtypeStruct(*out[i]) for i in indices]
            specs, aliases = [vmem] * len(indices), {}
            if part is not None:
                aliases = {len(sources): len(shapes)}
                sources += [whole, held(part)]
                shapes.append(jax.ShapeDtypeStruct(*out[fine]))
                specs = specs + [hbm, vmem]

            def body(*refs):
                ins, outs, sem = refs[: len(sources)], refs[len(sources) : -1], refs[-1]
                copies = [pltpu.make_async_copy(ins[i], outs[i], sem.at[i]) for i in range(len(indices))]
                if part is not None:
                    layer, first = place(lax.axis_index("dp"))
                    to = outs[-1].at[layer, pl.ds(pl.multiple_of(first, CORES * rows), CORES * rows), :]
                    copies.append(pltpu.make_async_copy(ins[-1], to, sem.at[len(indices)]))
                for copy in copies:
                    copy.start()
                for copy in copies:
                    copy.wait()

            moved = sum(x.size * x.dtype.itemsize for x in (*(results[i] for i in indices), *(() if part is None else (part,))))
            return pl.pallas_call(
                body,
                out_shape=shapes,
                in_specs=specs,
                out_specs=[hbm] * len(shapes),
                scratch_shapes=[dma((len(shapes),))],
                input_output_aliases=aliases,
                compiler_params=pltpu.CompilerParams(vmem_limit_bytes=VMEM_LIMIT),
                cost_estimate=pl.CostEstimate(flops=0, bytes_accessed=2 * moved, transcendentals=0),
            )(*sources)

        def place_of(me, core):
            far_chip = lax.rem(me // CORES + chips // 2, chips)
            return core * (layers // 2) + layers // 2 - 1, far_chip * CORES * rows

        own = lax.ppermute(tail, "dp", onward)
        first = list(range(6))
        done = dict(zip(first, write(first), strict=True))
        own, done[fine] = lax.optimization_barrier((own, done[fine]))
        mates_part = lax.ppermute(own, "dp", mates)
        later = list(range(6, 9))
        *got, whole = write(later, lambda me: place_of(me, lax.rem(me, CORES)), own, done[fine])
        done.update(zip(later, got, strict=True))
        (done[fine],) = write([], lambda me: place_of(me, 1 - lax.rem(me, CORES)), mates_part, whole)
        return tuple(done[i] for i in range(9))

    all_of, cut = P(None, None, None), P(None, "dp", None)
    return jax.shard_map(
        step,
        mesh=mesh,
        in_specs=(P(("rep", "dp"), None, None, None),) * 3 + (all_of,) * 3 + (cut,) * 6,
        out_specs=(P("rep", None, None),) * 3 + (P("rep", "dp", None),) * 6,
        check_vma=False,
    )
```

```python
import functools

import jax
import jax.numpy as jnp
from jax import lax
from jax.experimental import pallas as pl
from jax.experimental.pallas import tpu as pltpu
from jax.sharding import PartitionSpec as P

MESH = pl.DeviceIdType.MESH
CORES = 2
PIECES = 8
TILE = (16, 512)
WAYS = (0, 1)
F32, BF16 = jnp.float32, jnp.bfloat16
FIRST = range(8)
VMEM_LIMIT = 16 * 2**20


def kernel(n, fine, *refs):
    g, w, m_in, v_in, new, m, v = (refs[i : i + 3] for i in range(0, 21, 3))
    tail, last, *refs = refs[21:]
    far, near, own_w = (refs[i : i + 3] for i in range(0, 9, 3))
    (stage, acc, squares, term_sem, mate_sem, head_sem, stage_sem, state_sem, first_sem, second_sem, last_sem,
     back_sem, mate_send, back_send, sum_send, ring_send, square_sem, tail_sem) = refs[9:]

    chips = n // CORES
    me = lax.axis_index("dp")
    chip, core = me // CORES, me % CORES
    mate = chip * CORES + 1 - core
    right_chip, left_chip = lax.rem(chip + 1, chips), lax.rem(chip + chips - 1, chips)
    far_chip = lax.rem(chip + 2, chips)
    side = (right_chip * CORES + core, left_chip * CORES + core)
    layers = m[0].shape[0]
    half = layers // 2
    height = [ref.shape[1] for ref in m]
    arrays = [a for a in range(3) if a != fine] + [fine]
    steps = [(k, a, l) for k, (l, a) in enumerate((l, a) for l in range(half) for a in arrays)]
    final = len(steps) - 1
    head_first = steps[final:] + steps[:final]

    def to(device):
        return {"device_id": {"dp": device}, "device_id_type": MESH}

    def mine(c):
        return c * CORES + core

    def mates(c):
        return c * CORES + 1 - core

    def block(a, index, start=0, size=None):
        size = size or height[a]
        return pl.ds(pl.multiple_of(index * height[a] + start, size), size)

    def pieces(k, a, body):
        if k < final:
            body(0, 0, height[a])
        else:
            size = height[a] // PIECES
            pl.loop(0, PIECES)(lambda q: body(q, q * size, size))

    def tiles(a, size, body, carry):
        columns = m[a].shape[2] // TILE[1]

        def tile(i, carry):
            def at(base):
                r = pl.multiple_of(base + i // columns * TILE[0], TILE[0])
                return pl.ds(r, TILE[0]), pl.ds(pl.multiple_of(i % columns * TILE[1], TILE[1]), TILE[1])

            return body(at, carry)

        return lax.fori_loop(0, size // TILE[0] * columns, tile, carry)

    def drain(sem, ref):
        pltpu.make_async_copy(ref, ref, sem).wait()

    targets = (far_chip, right_chip, left_chip, chip)

    def term(t, a):
        where = block(a, mine(targets[t]))
        return pltpu.make_async_copy(g[a].at[0, :, where, :], new[a].at[:, where, :], term_sem.at[t, a])

    def mate_term(t, a):
        return pltpu.make_async_remote_copy(
            src_ref=g[a].at[0, :, block(a, mates(targets[t])), :], dst_ref=new[a].at[:, block(a, mine(targets[t])), :],
            send_sem=mate_send.at[a], recv_sem=mate_sem.at[t, a], **to(mate))

    def mate_head(q):
        size = height[fine] // PIECES
        return pltpu.make_async_remote_copy(
            src_ref=stage.at[:, block(fine, 0, q * size, size), :],
            dst_ref=new[fine].at[:, block(fine, mine(far_chip), q * size, size), :],
            send_sem=mate_send.at[fine], recv_sem=head_sem.at[q], **to(mate))

    to_stage = pltpu.make_async_copy(g[fine].at[0, :, block(fine, mates(far_chip)), :], stage, stage_sem.at[0])

    def states(a):
        return (pltpu.make_async_copy(m_in[a], m[a], state_sem.at[0, a]),
                pltpu.make_async_copy(v_in[a], v[a], state_sem.at[1, a]),
                pltpu.make_async_copy(w[a].at[:, block(a, me), :], own_w[a], state_sem.at[2, a]))

    barrier = pltpu.get_barrier_semaphore()
    for o in range(1, n):
        pl.semaphore_signal(barrier, inc=1, **to(lax.rem(me + o, n)))
    to_stage.start()
    for a in (fine, *arrays[:-1]):
        term(0, a).start()
    to_stage.wait()
    pl.semaphore_wait(barrier, n - 1)
    pl.loop(0, PIECES)(lambda q: mate_head(q).start())
    for t, a in [(0, a) for a in arrays[:-1]] + [(t, a) for a in arrays for t in (1, 2)] + [(3, a) for a in arrays]:
        mate_term(t, a).start()
        if t > 0:
            term(t, a).start()
    for a in arrays:
        for copy in states(a):
            copy.start()
    acc[...] = jnp.zeros_like(acc)

    arrived = set()

    def await_terms(t, a):
        if (t, a) not in arrived:
            arrived.add((t, a))
            term(t, a).wait()
            if (t, a) == (0, fine):
                return lambda q: mate_head(q).wait_recv()
            mate_term(t, a).wait_recv()
        return lambda q: None

    def total(t, a, layer, at, start, more):
        out = new[a][(layer, *at(mine(targets[t]) * height[a] + start))].astype(F32)
        out = out + new[a][(layer, *at(mates(targets[t]) * height[a] + start))].astype(F32)
        for ref, index in more:
            out = out + ref[(*index, *at(start))].astype(F32)
        return out

    def summed(t, a, layer, start, size, more=()):
        def tile(at, carry):
            new[a][(layer, *at(mine(targets[t]) * height[a] + start))] = total(t, a, layer, at, start, more).astype(BF16)
            return carry

        tiles(a, size, tile, 0)
        return new[a].at[layer, block(a, mine(targets[t]), start, size), :]

    def send_sum(way, a, src, dst, sem):
        pltpu.make_async_remote_copy(
            src_ref=src, dst_ref=dst, send_sem=sum_send.at[way, a], recv_sem=sem, **to(side[way])).start()

    def part(a, start, size):
        return pl.ds(pl.multiple_of(start, size), size)

    for k, a, l in head_first:
        here = await_terms(0, a)

        def body(q, start, size):
            here(q)
            for way in WAYS:
                src = summed(0, a, way * half + l, start, size)
                send_sum(way, a, src, far[a].at[way, l, part(a, start, size), :], first_sem.at[way, k])

        pieces(k, a, body)
    for k, a, l in steps:
        for way in WAYS:
            await_terms(1 + way, a)
            layer = (1 - way) * half + l
            src = summed(1 + way, a, layer, 0, height[a])
            send_sum(way, a, src, near[a].at[way, layer], second_sem.at[way, k])
    for k, a, l in steps:
        for way in WAYS:
            drain(first_sem.at[way, k], far[a].at[way, l])

        def body(q, start, size):
            for way in WAYS:
                layer = way * half + l
                src = summed(1 + way, a, layer, start, size, [(far[a], (way, l))])
                send_sum(way, a, src, near[a].at[way, layer, part(a, start, size), :], last_sem.at[way, k + q])

        pieces(k, a, body)
    for k, a, l in steps:
        await_terms(3, a)
        for way in WAYS:
            drain(second_sem.at[way, k], near[a].at[way, (1 - way) * half + l])

        def body(q, start, size):
            for way in WAYS:
                layer = way * half + l
                drain(last_sem.at[way, k + q], near[a].at[way, layer, part(a, start, size), :])

                def tile(at, carry):
                    rounded = total(3, a, layer, at, start, [(near[a], (i, layer)) for i in WAYS]).astype(BF16)
                    near[a][(0, layer, *at(start))] = rounded
                    rounded = rounded.astype(F32)
                    square = rounded * rounded
                    for r in range(0, TILE[0], 8):
                        for c in range(0, TILE[1], 128):
                            carry = carry + square[r : r + 8, c : c + 128]
                    return carry

                acc[...] = tiles(a, size, tile, acc[...])

        pieces(k, a, body)

    squares[me] = acc[...]
    for way in WAYS:
        for a in arrays:
            drain(sum_send.at[way, a], new[a].at[:half, pl.ds(0, 3 * height[a]), :])
    for o in range(1, n):
        pltpu.make_async_remote_copy(
            src_ref=squares.at[me], dst_ref=squares.at[me], send_sem=square_sem.at[0], recv_sem=square_sem.at[1],
            **to(lax.rem(me + o, n))).start()
    for a in arrays:
        for copy in states(a):
            copy.wait()
    drain(square_sem.at[1], squares.at[pl.ds(0, n - 1)])
    everyone = squares[0]
    for i in range(1, n):
        everyone = everyone + squares[i]
    everyone = jnp.sum(jnp.sum(everyone, axis=1, keepdims=True), axis=0, keepdims=True)
    count = n * sum(ref.size for ref in m)
    factor = jnp.minimum(1.0, 0.5 * lax.rsqrt(everyone / count + 1e-30))

    def ring(way, a, index, layer, start, size, sem):
        here = new[a].at[layer, block(a, index, start, size), :]
        pltpu.make_async_remote_copy(
            src_ref=here, dst_ref=here, send_sem=ring_send.at[way, a], recv_sem=sem, **to(side[way])).start()

    def back(a, index, layer, start, size):
        here = new[a].at[layer, block(a, index, start, size), :]
        pltpu.make_async_remote_copy(
            src_ref=here, dst_ref=here, send_sem=back_send.at[a], recv_sem=back_sem.at[a], **to(mate)).start()

    for k, a, l in head_first:
        def body(q, start, size):
            for way in WAYS:
                layer = way * half + l

                def tile(at, carry):
                    here = (layer, *at(start))
                    gradient = near[a][(0, *here)].astype(F32) * factor
                    mean = 0.9 * m[a][here] + 0.1 * gradient
                    variance = 0.95 * v[a][here] + 0.05 * gradient * gradient
                    weight = own_w[a][here].astype(F32)
                    step = mean * lax.rsqrt(variance + 1e-8) + 0.1 * weight
                    m[a][here] = mean
                    v[a][here] = variance
                    new[a][(layer, *at(me * height[a] + start))] = (weight - 0.02 * step).astype(BF16)
                    return carry

                tiles(a, size, tile, 0)
                ring(way, a, me, layer, start, size, first_sem.at[way, k])
                back(a, me, layer, start, size)

        pieces(k, a, body)
    for k, a, l in steps:
        for way in WAYS:
            ring(way, a, me, (1 - way) * half + l, 0, height[a], second_sem.at[way, k])
    source = (mine(left_chip), mine(right_chip))
    for k, a, l in head_first:
        for way in WAYS:
            layer = way * half + l
            drain(first_sem.at[way, k], new[a].at[layer, block(a, source[way]), :])
            if k < final:
                back(a, source[way], layer, 0, height[a])
            else:
                here = new[a].at[layer, block(a, source[way]), :]
                pltpu.make_async_remote_copy(
                    src_ref=here, dst_ref=here, send_sem=tail_sem.at[2], recv_sem=tail_sem.at[way], **to(mate)).start()

    for k, a, l in steps[:final]:
        for way in WAYS:
            here = new[a].at[way * half + l, block(a, source[way]), :]
            there = last.at[way] if k == final - 1 else here
            pltpu.make_async_remote_copy(
                src_ref=here, dst_ref=there, send_sem=ring_send.at[way, a], recv_sem=last_sem.at[way, k], **to(side[way])).start()
    for k, a, l in steps:
        for way in WAYS:
            layer = (1 - way) * half + l
            drain(second_sem.at[way, k], new[a].at[layer, block(a, source[way]), :])
            back(a, source[way], layer, 0, height[a])
    _, a, l = steps[final]
    for way in WAYS:
        drain(tail_sem.at[way], new[a].at[way * half + l, block(a, mates((left_chip, right_chip)[way])), :])
    pair = CORES * height[a]
    where = pl.ds(pl.multiple_of((left_chip + core * (right_chip - left_chip)) * pair, pair), pair)
    to_tail = pltpu.make_async_copy(new[a].at[core * half + l, where, :], tail, tail_sem.at[3])
    to_tail.start()
    for k, a, l in steps[: final - 1]:
        for way in WAYS:
            layer = way * half + l
            drain(last_sem.at[way, k], new[a].at[layer, block(a, mine(far_chip)), :])
            back(a, mine(far_chip), layer, 0, height[a])
    to_tail.wait()
    drain(tail_sem.at[2], new[fine].at[0, pl.ds(0, 2 * height[fine]), :])
    for a in arrays:
        drain(mate_send.at[a], new[a].at[:half])
        blocks = (4 * layers - (4 if a == fine else 2 if a == steps[final - 1][1] else 0)) // half
        for sem in (back_send, back_sem):
            drain(sem.at[a], new[a].at[:half, pl.ds(0, blocks * height[a]), :])
        for way in WAYS:
            blocks = 3 * half - (a == fine)
            drain(ring_send.at[way, a], new[a].at[0, pl.ds(0, blocks * height[a]), :])
    for way in WAYS:
        drain(last_sem.at[way, final - 1], last.at[way])
    drain(square_sem.at[0], squares.at[pl.ds(0, n - 1)])


def solution(mesh):
    n = mesh.shape["dp"]
    chips = n // CORES
    onward = [(i, (i // CORES + (1 if i % CORES == 0 else chips - 1)) % chips * CORES + 1 - i % CORES) for i in range(n)]
    mates = [(i, i // CORES * CORES + 1 - i % CORES) for i in range(n)]

    def step(*arrays):
        terms, weights, m, v = (arrays[i : i + 3] for i in (0, 3, 6, 9))
        layers = m[0].shape[0]
        hbm = pl.BlockSpec(memory_space=pltpu.HBM)
        vmem = pl.BlockSpec(memory_space=pltpu.VMEM)
        dma = pltpu.SemaphoreType.DMA
        blocks = [one.shape[1:] for one in m]
        fine = max(range(3), key=lambda a: blocks[a][0])
        out = [(w.shape, BF16) for w in weights] + [(x.shape, F32) for x in (*m, *v)]
        steps = 3 * (layers // 2)
        rows, columns = blocks[fine]
        scratch = (
            [pltpu.VMEM((2, layers // 2, *b), BF16) for b in blocks]
            + [pltpu.VMEM((2, layers, *b), BF16) for b in blocks]
            + [pltpu.VMEM((layers, *b), BF16) for b in blocks]
            + [pltpu.VMEM((layers, *blocks[fine]), BF16), pltpu.VMEM((8, 128), F32), pltpu.VMEM((n, 8, 128), F32)]
            + [dma((4, 3)), dma((4, 3)), dma((PIECES,)), dma((1,)), dma((3, 3))]
            + [dma((2, steps)), dma((2, steps)), dma((2, steps - 1 + PIECES))]
            + [dma((3,)), dma((3,)), dma((3,)), dma((2, 3)), dma((2, 3)), dma((2,)), dma((4,))]
        )
        late = [a for a in range(3) if a != fine][-1]
        *results, tail, last = pl.pallas_call(
            functools.partial(kernel, n, fine),
            out_shape=[pltpu.VMEM(shape, dtype) for shape, dtype in [*out, ((CORES * rows, columns), BF16), ((2, *blocks[late]), BF16)]],
            in_specs=[hbm] * len(arrays),
            out_specs=[vmem] * (len(out) + 2),
            scratch_shapes=scratch,
            compiler_params=pltpu.CompilerParams(
                collective_id=0, has_side_effects=True, vmem_limit_bytes=VMEM_LIMIT),
        )(*arrays)

        def write(done, indices, patches=()):
            held = [pltpu.with_memory_space_constraint(x, pltpu.VMEM) for x in (*(results[i] for i in indices), *(p[1] for p in patches))]
            changed = sorted({p[0] for p in patches})
            written = [*changed, *indices]

            def body(*refs):
                olds, refs = refs[: len(changed)], refs[len(changed) :]
                ins, outs, sem = refs[: len(held)], dict(zip(written, refs[len(held) : -1], strict=True)), refs[-1]
                to = [outs[i] for i in indices] + [place(outs[i]) for i, _, place in patches]
                copies = [pltpu.make_async_copy(x, y, sem.at[i]) for i, (x, y) in enumerate(zip(ins, to, strict=True))]
                for copy in copies:
                    copy.start()
                for copy in copies:
                    copy.wait()

            fresh = pl.pallas_call(
                body,
                out_shape=[jax.ShapeDtypeStruct(*out[i]) for i in written],
                in_specs=[hbm] * len(changed) + [vmem] * len(held),
                out_specs=[hbm] * len(written),
                scratch_shapes=[dma((len(held),))],
                input_output_aliases={i: i for i in range(len(changed))},
                compiler_params=pltpu.CompilerParams(vmem_limit_bytes=VMEM_LIMIT),
                cost_estimate=pl.CostEstimate(
                    flops=0, bytes_accessed=2 * sum(x.size * x.dtype.itemsize for x in held), transcendentals=0),
            )(*(done[i] for i in changed), *held)
            done.update(zip(written, fresh, strict=True))

        def far_rows(of_mate):
            me = lax.axis_index("dp")
            core = me % CORES
            return lax.rem(me // CORES + chips // 2, chips), (1 - core if of_mate else core)

        def from_tail(of_mate):
            def place(ref):
                far_chip, core = far_rows(of_mate)
                pair = CORES * rows
                return ref.at[(CORES - core) * (layers // 2) - 1, pl.ds(pl.multiple_of(far_chip * pair, pair), pair), :]

            return place

        def from_last(of_mate):
            def place(ref):
                far_chip, core = far_rows(of_mate)
                size = blocks[late][0]
                return ref.at[layers // 2 - 1 :: layers // 2, pl.ds(pl.multiple_of((far_chip * CORES + core) * size, size), size), :]

            return place

        done = {}
        own = lax.ppermute(tail, "dp", onward)
        mates_last = lax.ppermute(last, "dp", mates)
        write(done, FIRST)
        own, done[fine] = lax.optimization_barrier((own, done[fine]))
        mates_own = lax.ppermute(own, "dp", mates)
        write(done, [i for i in range(9) if i not in FIRST],
              [(fine, own, from_tail(False)), (late, last, from_last(False)), (late, mates_last, from_last(True))])
        write(done, [], [(fine, mates_own, from_tail(True))])
        return tuple(done[i] for i in range(9))

    all_of, cut = P(None, None, None), P(None, "dp", None)
    return jax.shard_map(
        step,
        mesh=mesh,
        in_specs=(P(("rep", "dp"), None, None, None),) * 3 + (all_of,) * 3 + (cut,) * 6,
        out_specs=(P("rep", None, None),) * 3 + (P("rep", "dp", None),) * 6,
        check_vma=False,
    )
```

```python
import functools
import math

import jax
import jax.numpy as jnp
from jax import lax
from jax.experimental import pallas as pl
from jax.experimental.pallas import tpu as pltpu
from jax.sharding import PartitionSpec as P

MESH = pl.DeviceIdType.MESH
CORES = 2
PIECES = (16, 16, 8, 4, 2)
TILE = (16, 512)
WAYS = (0, 1)
F32, BF16 = jnp.float32, jnp.bfloat16
FIRST = range(8)
VMEM_LIMIT = 16 * 2**20


def kernel(n, fine, *refs):
    g, w, m_in, v_in, new, m, v = (refs[i : i + 3] for i in range(0, 21, 3))
    tail, last, *refs = refs[21:]
    far, near, own_w = (refs[i : i + 3] for i in range(0, 9, 3))
    (stage, acc, squares, load_sem, mate_sem, head_sem, stage_sem, first_sem, second_sem, last_sem, back_sem, mate_send,
     back_send, sum_send, ring_send, square_sem, tail_sem) = refs[9:]

    chips = n // CORES
    me = lax.axis_index("dp")
    chip, core = me // CORES, me % CORES
    mate = chip * CORES + 1 - core
    right_chip, left_chip = lax.rem(chip + 1, chips), lax.rem(chip + chips - 1, chips)
    far_chip = lax.rem(chip + 2, chips)
    side = (right_chip * CORES + core, left_chip * CORES + core)
    layers = m[0].shape[0]
    half = layers // 2
    height = [ref.shape[1] for ref in m]
    arrays = [a for a in range(3) if a != fine] + [fine]
    steps = [(k, a, l) for k, (l, a) in enumerate((l, a) for l in range(half) for a in arrays)]
    final = len(steps) - 1
    head_first = steps[final:] + steps[:final]

    def to(device):
        return {"device_id": {"dp": device}, "device_id_type": MESH}

    def mine(c):
        return c * CORES + core

    def mates(c):
        return c * CORES + 1 - core

    def block(a, index, start=0, size=None):
        size = size or height[a]
        return pl.ds(pl.multiple_of(index * height[a] + start, math.gcd(height[a], start)), size)

    def pieces(k, a, order=1):
        sizes = [height[a] // p for p in PIECES[::order]] if k == final else [height[a]]
        return [(q, sum(sizes[:q]), size) for q, size in enumerate(sizes)]

    head = pieces(final, fine)

    def tiles(a, size, body, carry):
        columns = m[a].shape[2] // TILE[1]

        def tile(i, carry):
            def at(base):
                r = pl.multiple_of(base + i // columns * TILE[0], TILE[0])
                return pl.ds(r, TILE[0]), pl.ds(pl.multiple_of(i % columns * TILE[1], TILE[1]), TILE[1])

            return body(at, carry)

        return lax.fori_loop(0, size // TILE[0] * columns, tile, carry)

    def drain(sem, ref):
        pltpu.make_async_copy(ref, ref, sem).wait()

    targets = (far_chip, right_chip, left_chip, chip)

    def group(t, a):
        return (0 if a == fine else 1) if t == 0 else 2 if t < 3 else 3

    def term(t, a):
        where = block(a, mine(targets[t]))
        return pltpu.make_async_copy(g[a].at[0, :, where, :], new[a].at[:, where, :], load_sem.at[group(t, a)])

    def mate_term(t, a):
        return pltpu.make_async_remote_copy(
            src_ref=g[a].at[0, :, block(a, mates(targets[t])), :], dst_ref=new[a].at[:, block(a, mine(targets[t])), :],
            send_sem=mate_send.at[a], recv_sem=mate_sem.at[group(t, a)], **to(mate))

    def mate_head(q, start, size):
        return pltpu.make_async_remote_copy(
            src_ref=stage.at[:, pl.ds(start, size), :],
            dst_ref=new[fine].at[:, block(fine, mine(far_chip), start, size), :],
            send_sem=mate_send.at[fine], recv_sem=head_sem.at[q], **to(mate))

    def to_stage(q, start, size):
        return pltpu.make_async_copy(
            g[fine].at[0, :, block(fine, mates(far_chip), start, size), :], stage.at[:, pl.ds(start, size), :], stage_sem.at[q])

    staged = [(0, *head[0][1:]), (1, head[1][1], height[fine] - head[1][1])]

    def states(a):
        return (pltpu.make_async_copy(m_in[a], m[a], load_sem.at[4]),
                pltpu.make_async_copy(v_in[a], v[a], load_sem.at[5]),
                pltpu.make_async_copy(w[a].at[:, block(a, me), :], own_w[a], load_sem.at[6]))

    for q, start, size in staged:
        to_stage(q, start, size).start()
    barrier = pltpu.get_barrier_semaphore()
    for o in range(1, n):
        pl.semaphore_signal(barrier, inc=1, **to(lax.rem(me + o, n)))
    for a in (fine, *arrays[:-1]):
        term(0, a).start()
    to_stage(*staged[0]).wait()
    pl.semaphore_wait(barrier, n - 1)
    mate_head(*head[0]).start()
    to_stage(*staged[1]).wait()
    for piece in head[1:]:
        mate_head(*piece).start()
    for t, a in [(0, a) for a in arrays[:-1]] + [(t, a) for a in arrays for t in (1, 2)] + [(3, a) for a in arrays]:
        mate_term(t, a).start()
        if t > 0:
            term(t, a).start()
    for a in arrays:
        for copy in states(a):
            copy.start()
    acc[...] = jnp.zeros_like(acc)

    def drain_blocks(sem, count):
        drain(sem, new[fine].at[:, pl.ds(0, count * height[fine] // layers), :])

    arrived = set()

    def await_terms(t, a):
        i = group(t, a)
        if i not in arrived:
            arrived.add(i)
            count = layers * sum(group(t, a) == i for t in range(4) for a in arrays)
            drain_blocks(load_sem.at[i], count)
            if i > 0:
                drain_blocks(mate_sem.at[i], count)

    def total(t, a, layer, at, start, more):
        out = new[a][(layer, *at(mine(targets[t]) * height[a] + start))].astype(F32)
        out = out + new[a][(layer, *at(mates(targets[t]) * height[a] + start))].astype(F32)
        for ref, index in more:
            out = out + ref[(*index, *at(start))].astype(F32)
        return out

    def summed(t, a, layer, start, size, more=()):
        def tile(at, carry):
            new[a][(layer, *at(mine(targets[t]) * height[a] + start))] = total(t, a, layer, at, start, more).astype(BF16)
            return carry

        tiles(a, size, tile, 0)
        return new[a].at[layer, block(a, mine(targets[t]), start, size), :]

    def send_sum(way, a, src, dst, sem):
        pltpu.make_async_remote_copy(
            src_ref=src, dst_ref=dst, send_sem=sum_send.at[a], recv_sem=sem, **to(side[way])).start()

    for k, a, l in head_first:
        await_terms(0, a)
        for q, start, size in pieces(k, a):
            if a == fine and k == final:
                mate_head(q, start, size).wait_recv()
            for way in WAYS:
                src = summed(0, a, way * half + l, start, size)
                send_sum(way, a, src, far[a].at[way, l, pl.ds(start, size), :], first_sem.at[k])
    for k, a, l in steps:
        for way in WAYS:
            await_terms(1 + way, a)
            layer = (1 - way) * half + l
            src = summed(1 + way, a, layer, 0, height[a])
            send_sum(way, a, src, near[a].at[way, layer], second_sem.at[k])
    for k, a, l in steps:
        drain(first_sem.at[k], far[a].at[:, l])
        for q, start, size in pieces(k, a, -1):
            for way in WAYS:
                layer = way * half + l
                src = summed(1 + way, a, layer, start, size, [(far[a], (way, l))])
                send_sum(way, a, src, near[a].at[way, layer, pl.ds(start, size), :], last_sem.at[k + q])
    for k, a, l in steps:
        await_terms(3, a)
        drain(second_sem.at[k], far[a].at[:, l])
        for q, start, size in pieces(k, a, -1):
            drain(last_sem.at[k + q], far[a].at[:, l, pl.ds(start, size), :])
            for way in WAYS:
                layer = way * half + l

                def tile(at, carry):
                    rounded = total(3, a, layer, at, start, [(near[a], (i, layer)) for i in WAYS]).astype(BF16)
                    near[a][(0, layer, *at(start))] = rounded
                    rounded = rounded.astype(F32)
                    square = rounded * rounded
                    for r in range(0, TILE[0], 8):
                        for c in range(0, TILE[1], 128):
                            carry = carry + square[r : r + 8, c : c + 128]
                    return carry

                acc[...] = tiles(a, size, tile, acc[...])

    squares[me] = acc[...]
    for a in arrays:
        drain_blocks(sum_send.at[a], 3 * layers)
    for o in range(1, n):
        pltpu.make_async_remote_copy(
            src_ref=squares.at[me], dst_ref=squares.at[me], send_sem=square_sem.at[0], recv_sem=square_sem.at[1],
            **to(lax.rem(me + o, n))).start()
    for i, ref in ((4, F32), (5, F32), (6, BF16)):
        drain_blocks(load_sem.at[i], len(arrays) * layers * (2 if ref == F32 else 1))
    drain(square_sem.at[1], squares.at[pl.ds(0, n - 1)])
    everyone = squares[0]
    for i in range(1, n):
        everyone = everyone + squares[i]
    everyone = jnp.sum(jnp.sum(everyone, axis=1, keepdims=True), axis=0, keepdims=True)
    count = n * sum(ref.size for ref in m)
    factor = jnp.minimum(1.0, 0.5 * lax.rsqrt(everyone / count + 1e-30))

    def ring(way, a, index, layer, start, size, sem):
        here = new[a].at[layer, block(a, index, start, size), :]
        pltpu.make_async_remote_copy(
            src_ref=here, dst_ref=here, send_sem=ring_send.at[a], recv_sem=sem, **to(side[way])).start()

    def back(a, index, layer, start, size):
        here = new[a].at[layer, block(a, index, start, size), :]
        pltpu.make_async_remote_copy(
            src_ref=here, dst_ref=here, send_sem=back_send.at[a], recv_sem=back_sem.at[a], **to(mate)).start()

    for k, a, l in head_first:
        for q, start, size in pieces(k, a):
            for way in WAYS:
                layer = way * half + l

                def tile(at, carry):
                    here = (layer, *at(start))
                    gradient = near[a][(0, *here)].astype(F32) * factor
                    mean = 0.9 * m[a][here] + 0.1 * gradient
                    variance = 0.95 * v[a][here] + 0.05 * gradient * gradient
                    weight = own_w[a][here].astype(F32)
                    step = mean * lax.rsqrt(variance + 1e-8) + 0.1 * weight
                    m[a][here] = mean
                    v[a][here] = variance
                    new[a][(layer, *at(me * height[a] + start))] = (weight - 0.02 * step).astype(BF16)
                    return carry

                tiles(a, size, tile, 0)
                ring(way, a, me, layer, start, size, first_sem.at[k])
                back(a, me, layer, start, size)
    for k, a, l in steps:
        for way in WAYS:
            ring(way, a, me, (1 - way) * half + l, 0, height[a], second_sem.at[k])
    source = (mine(left_chip), mine(right_chip))
    for k, a, l in head_first:
        drain(first_sem.at[k], far[a].at[:, l])
        for way in WAYS:
            layer = way * half + l
            if k < final:
                back(a, source[way], layer, 0, height[a])
            else:
                here = new[a].at[layer, block(a, source[way]), :]
                pltpu.make_async_remote_copy(
                    src_ref=here, dst_ref=here, send_sem=tail_sem.at[2], recv_sem=tail_sem.at[way], **to(mate)).start()

    for k, a, l in steps[:final]:
        for way in WAYS:
            here = new[a].at[way * half + l, block(a, source[way]), :]
            there = last.at[way] if k == final - 1 else here
            pltpu.make_async_remote_copy(
                src_ref=here, dst_ref=there, send_sem=ring_send.at[a], recv_sem=last_sem.at[k], **to(side[way])).start()
    for k, a, l in steps:
        drain(second_sem.at[k], far[a].at[:, l])
        for way in WAYS:
            layer = (1 - way) * half + l
            back(a, source[way], layer, 0, height[a])
    _, a, l = steps[final]
    for way in WAYS:
        drain(tail_sem.at[way], new[a].at[way * half + l, block(a, mates((left_chip, right_chip)[way])), :])
    pair = CORES * height[a]
    where = pl.ds(pl.multiple_of((left_chip + core * (right_chip - left_chip)) * pair, pair), pair)
    to_tail = pltpu.make_async_copy(new[a].at[core * half + l, where, :], tail, tail_sem.at[3])
    to_tail.start()
    for k, a, l in steps[: final - 1]:
        drain(last_sem.at[k], far[a].at[:, l])
        for way in WAYS:
            layer = way * half + l
            back(a, mine(far_chip), layer, 0, height[a])
    to_tail.wait()
    drain(tail_sem.at[2], new[fine].at[0, pl.ds(0, 2 * height[fine]), :])
    for a in arrays:
        drain(mate_send.at[a], new[a].at[:half])
        blocks = (4 * layers - (4 if a == fine else 2 if a == steps[final - 1][1] else 0)) // half
        for sem in (back_send, back_sem):
            drain(sem.at[a], new[a].at[:half, pl.ds(0, blocks * height[a]), :])
        drain_blocks(ring_send.at[a], 3 * layers - (2 if a == fine else 0))
    drain(last_sem.at[final - 1], last)
    drain(square_sem.at[0], squares.at[pl.ds(0, n - 1)])


def solution(mesh):
    n = mesh.shape["dp"]
    chips = n // CORES
    onward = [(i, (i // CORES + (1 if i % CORES == 0 else chips - 1)) % chips * CORES + 1 - i % CORES) for i in range(n)]
    mates = [(i, i // CORES * CORES + 1 - i % CORES) for i in range(n)]

    def step(*arrays):
        terms, weights, m, v = (arrays[i : i + 3] for i in (0, 3, 6, 9))
        layers = m[0].shape[0]
        hbm = pl.BlockSpec(memory_space=pltpu.HBM)
        vmem = pl.BlockSpec(memory_space=pltpu.VMEM)
        dma = pltpu.SemaphoreType.DMA
        blocks = [one.shape[1:] for one in m]
        fine = max(range(3), key=lambda a: blocks[a][0])
        out = [(w.shape, BF16) for w in weights] + [(x.shape, F32) for x in (*m, *v)]
        steps = 3 * (layers // 2)
        rows, columns = blocks[fine]
        scratch = (
            [pltpu.VMEM((2, layers // 2, *b), BF16) for b in blocks]
            + [pltpu.VMEM((2, layers, *b), BF16) for b in blocks]
            + [pltpu.VMEM((layers, *b), BF16) for b in blocks]
            + [pltpu.VMEM((layers, *blocks[fine]), BF16), pltpu.VMEM((8, 128), F32), pltpu.VMEM((n, 8, 128), F32)]
            + [dma((7,)), dma((4,)), dma((len(PIECES),)), dma((2,))]
            + [dma((steps,)), dma((steps,)), dma((steps - 1 + len(PIECES),))]
            + [dma((3,)), dma((3,)), dma((3,)), dma((3,)), dma((3,)), dma((2,)), dma((4,))]
        )
        late = [a for a in range(3) if a != fine][-1]
        *results, tail, last = pl.pallas_call(
            functools.partial(kernel, n, fine),
            out_shape=[pltpu.VMEM(shape, dtype) for shape, dtype in [*out, ((CORES * rows, columns), BF16), ((2, *blocks[late]), BF16)]],
            in_specs=[hbm] * len(arrays),
            out_specs=[vmem] * (len(out) + 2),
            scratch_shapes=scratch,
            compiler_params=pltpu.CompilerParams(
                collective_id=0, has_side_effects=True, vmem_limit_bytes=VMEM_LIMIT),
        )(*arrays)

        def write(done, indices, patches=()):
            held = [pltpu.with_memory_space_constraint(x, pltpu.VMEM) for x in (*(results[i] for i in indices), *(p[1] for p in patches))]
            changed = sorted({p[0] for p in patches})
            written = [*changed, *indices]

            def body(*refs):
                olds, refs = refs[: len(changed)], refs[len(changed) :]
                ins, outs, sem = refs[: len(held)], dict(zip(written, refs[len(held) : -1], strict=True)), refs[-1]
                to = [outs[i] for i in indices] + [place(outs[i]) for i, _, place in patches]
                copies = [pltpu.make_async_copy(x, y, sem.at[i]) for i, (x, y) in enumerate(zip(ins, to, strict=True))]
                for copy in copies:
                    copy.start()
                for copy in copies:
                    copy.wait()

            fresh = pl.pallas_call(
                body,
                out_shape=[jax.ShapeDtypeStruct(*out[i]) for i in written],
                in_specs=[hbm] * len(changed) + [vmem] * len(held),
                out_specs=[hbm] * len(written),
                scratch_shapes=[dma((len(held),))],
                input_output_aliases={i: i for i in range(len(changed))},
                compiler_params=pltpu.CompilerParams(vmem_limit_bytes=VMEM_LIMIT),
                cost_estimate=pl.CostEstimate(
                    flops=0, bytes_accessed=2 * sum(x.size * x.dtype.itemsize for x in held), transcendentals=0),
            )(*(done[i] for i in changed), *held)
            done.update(zip(written, fresh, strict=True))

        def far_rows(of_mate):
            me = lax.axis_index("dp")
            core = me % CORES
            return lax.rem(me // CORES + chips // 2, chips), (1 - core if of_mate else core)

        def from_tail(of_mate):
            def place(ref):
                far_chip, core = far_rows(of_mate)
                pair = CORES * rows
                return ref.at[(CORES - core) * (layers // 2) - 1, pl.ds(pl.multiple_of(far_chip * pair, pair), pair), :]

            return place

        def from_last(of_mate):
            def place(ref):
                far_chip, core = far_rows(of_mate)
                size = blocks[late][0]
                return ref.at[layers // 2 - 1 :: layers // 2, pl.ds(pl.multiple_of((far_chip * CORES + core) * size, size), size), :]

            return place

        done = {}
        own = lax.ppermute(tail, "dp", onward)
        mates_last = lax.ppermute(last, "dp", mates)
        write(done, FIRST)
        own, done[fine] = lax.optimization_barrier((own, done[fine]))
        mates_own = lax.ppermute(own, "dp", mates)
        write(done, [i for i in range(9) if i not in FIRST],
              [(fine, own, from_tail(False)), (late, last, from_last(False)), (late, mates_last, from_last(True))])
        write(done, [], [(fine, mates_own, from_tail(True))])
        return tuple(done[i] for i in range(9))

    all_of, cut = P(None, None, None), P(None, "dp", None)
    return jax.shard_map(
        step,
        mesh=mesh,
        in_specs=(P(("rep", "dp"), None, None, None),) * 3 + (all_of,) * 3 + (cut,) * 6,
        out_specs=(P("rep", None, None),) * 3 + (P("rep", "dp", None),) * 6,
        check_vma=False,
    )
```

```python
import functools
import math

import jax
import jax.numpy as jnp
from jax import lax
from jax.experimental import pallas as pl
from jax.experimental.pallas import tpu as pltpu
from jax.sharding import PartitionSpec as P

MESH = pl.DeviceIdType.MESH
CORES = 2
PIECES = (16, 16, 8, 4, 2)
HOLD = ((0, 3300), (800, 0))
TILE = (16, 512)
WAYS = (0, 1)
F32, BF16 = jnp.float32, jnp.bfloat16
FIRST = range(8)
VMEM_LIMIT = 16 * 2**20


def kernel(n, fine, *refs):
    g, w, m_in, v_in, new, m, v = (refs[i : i + 3] for i in range(0, 21, 3))
    tail, last, *refs = refs[21:]
    far, near, own_w = (refs[i : i + 3] for i in range(0, 9, 3))
    (stage, acc, squares, load_sem, mate_sem, head_sem, stage_sem, first_sem, second_sem, last_sem, back_sem, mate_send,
     back_send, sum_send, ring_send, square_sem, tail_sem) = refs[9:]

    chips = n // CORES
    me = lax.axis_index("dp")
    chip, core = me // CORES, me % CORES
    mate = chip * CORES + 1 - core
    right_chip, left_chip = lax.rem(chip + 1, chips), lax.rem(chip + chips - 1, chips)
    far_chip = lax.rem(chip + 2, chips)
    side = (right_chip * CORES + core, left_chip * CORES + core)
    layers = m[0].shape[0]
    half = layers // 2
    height = [ref.shape[1] for ref in m]
    arrays = [a for a in range(3) if a != fine] + [fine]
    steps = [(k, a, l) for k, (l, a) in enumerate((l, a) for l in range(half) for a in arrays)]
    final = len(steps) - 1
    head_first = steps[final:] + steps[:final]

    def to(device):
        return {"device_id": {"dp": device}, "device_id_type": MESH}

    def mine(c):
        return c * CORES + core

    def mates(c):
        return c * CORES + 1 - core

    def block(a, index, start=0, size=None):
        size = size or height[a]
        return pl.ds(pl.multiple_of(index * height[a] + start, math.gcd(height[a], start)), size)

    def pieces(k, a, order=1):
        sizes = [height[a] // p for p in PIECES[::order]] if k == final else [height[a]]
        return [(q, sum(sizes[:q]), size) for q, size in enumerate(sizes)]

    head = pieces(final, fine)

    def tiles(a, size, body, carry):
        columns = m[a].shape[2] // TILE[1]

        def tile(i, carry):
            def at(base):
                r = pl.multiple_of(base + i // columns * TILE[0], TILE[0])
                return pl.ds(r, TILE[0]), pl.ds(pl.multiple_of(i % columns * TILE[1], TILE[1]), TILE[1])

            return body(at, carry)

        return lax.fori_loop(0, size // TILE[0] * columns, tile, carry)

    def drain(sem, ref):
        pltpu.make_async_copy(ref, ref, sem).wait()

    targets = (far_chip, right_chip, left_chip, chip)

    def group(t, a):
        return (0 if a == fine else 1) if t == 0 else 2 if t < 3 else 3

    def term(t, a):
        where = block(a, mine(targets[t]))
        return pltpu.make_async_copy(g[a].at[0, :, where, :], new[a].at[:, where, :], load_sem.at[group(t, a)])

    def mate_term(t, a):
        return pltpu.make_async_remote_copy(
            src_ref=g[a].at[0, :, block(a, mates(targets[t])), :], dst_ref=new[a].at[:, block(a, mine(targets[t])), :],
            send_sem=mate_send.at[a], recv_sem=mate_sem.at[group(t, a)], **to(mate))

    def mate_head(q, start, size):
        return pltpu.make_async_remote_copy(
            src_ref=stage.at[:, pl.ds(start, size), :],
            dst_ref=new[fine].at[:, block(fine, mine(far_chip), start, size), :],
            send_sem=mate_send.at[fine], recv_sem=head_sem.at[q], **to(mate))

    def to_stage(q, start, size):
        return pltpu.make_async_copy(
            g[fine].at[0, :, block(fine, mates(far_chip), start, size), :], stage.at[:, pl.ds(start, size), :], stage_sem.at[q])

    staged = [(0, *head[0][1:]), (1, head[1][1], height[fine] - head[1][1])]

    def states(a):
        return (pltpu.make_async_copy(m_in[a], m[a], load_sem.at[4]),
                pltpu.make_async_copy(v_in[a], v[a], load_sem.at[5]),
                pltpu.make_async_copy(w[a].at[:, block(a, me), :], own_w[a], load_sem.at[6]))

    for q, start, size in staged:
        to_stage(q, start, size).start()
    barrier = pltpu.get_barrier_semaphore()
    for o in range(1, n):
        pl.semaphore_signal(barrier, inc=1, **to(lax.rem(me + o, n)))
    for a in (fine, *arrays[:-1]):
        term(0, a).start()
    to_stage(*staged[0]).wait()
    pl.semaphore_wait(barrier, n - 1)
    mate_head(*head[0]).start()
    to_stage(*staged[1]).wait()
    for piece in head[1:]:
        mate_head(*piece).start()
    for t, a in [(0, a) for a in arrays[:-1]] + [(t, a) for a in arrays for t in (1, 2)] + [(3, a) for a in arrays]:
        mate_term(t, a).start()
        if t > 0:
            term(t, a).start()
    for a in arrays:
        for copy in states(a):
            copy.start()
    acc[...] = jnp.zeros_like(acc)

    def drain_blocks(sem, count):
        drain(sem, new[fine].at[:, pl.ds(0, count * height[fine] // layers), :])

    arrived = set()

    def await_terms(t, a):
        i = group(t, a)
        if i not in arrived:
            arrived.add(i)
            count = layers * sum(group(t, a) == i for t in range(4) for a in arrays)
            drain_blocks(load_sem.at[i], count)
            if i > 0:
                drain_blocks(mate_sem.at[i], count)

    def total(t, a, layer, at, start, more):
        out = new[a][(layer, *at(mine(targets[t]) * height[a] + start))].astype(F32)
        out = out + new[a][(layer, *at(mates(targets[t]) * height[a] + start))].astype(F32)
        for ref, index in more:
            out = out + ref[(*index, *at(start))].astype(F32)
        return out

    def summed(t, a, layer, start, size, more=()):
        def tile(at, carry):
            new[a][(layer, *at(mine(targets[t]) * height[a] + start))] = total(t, a, layer, at, start, more).astype(BF16)
            return carry

        tiles(a, size, tile, 0)
        return new[a].at[layer, block(a, mine(targets[t]), start, size), :]

    def send_sum(way, a, src, dst, sem):
        pltpu.make_async_remote_copy(
            src_ref=src, dst_ref=dst, send_sem=sum_send.at[a], recv_sem=sem, **to(side[way])).start()

    def hold(phase):
        for index, time in enumerate(HOLD[phase]):
            if time:
                pl.when(core == index)(lambda: pl.delay(time))

    hold(0)
    for k, a, l in head_first:
        await_terms(0, a)
        for q, start, size in pieces(k, a):
            if a == fine and k == final:
                mate_head(q, start, size).wait_recv()
            for way in WAYS:
                src = summed(0, a, way * half + l, start, size)
                send_sum(way, a, src, far[a].at[way, l, pl.ds(start, size), :], first_sem.at[k])
    for k, a, l in steps:
        for way in WAYS:
            await_terms(1 + way, a)
            layer = (1 - way) * half + l
            src = summed(1 + way, a, layer, 0, height[a])
            send_sum(way, a, src, near[a].at[way, layer], second_sem.at[k])
    for k, a, l in steps:
        drain(first_sem.at[k], far[a].at[:, l])
        for q, start, size in pieces(k, a, -1):
            for way in WAYS:
                layer = way * half + l
                src = summed(1 + way, a, layer, start, size, [(far[a], (way, l))])
                send_sum(way, a, src, near[a].at[way, layer, pl.ds(start, size), :], last_sem.at[k + q])
    for k, a, l in steps:
        await_terms(3, a)
        drain(second_sem.at[k], far[a].at[:, l])
        for q, start, size in pieces(k, a, -1):
            drain(last_sem.at[k + q], far[a].at[:, l, pl.ds(start, size), :])
            for way in WAYS:
                layer = way * half + l

                def tile(at, carry):
                    rounded = total(3, a, layer, at, start, [(near[a], (i, layer)) for i in WAYS]).astype(BF16)
                    near[a][(0, layer, *at(start))] = rounded
                    rounded = rounded.astype(F32)
                    square = rounded * rounded
                    for r in range(0, TILE[0], 8):
                        for c in range(0, TILE[1], 128):
                            carry = carry + square[r : r + 8, c : c + 128]
                    return carry

                acc[...] = tiles(a, size, tile, acc[...])

    squares[me] = acc[...]
    for a in arrays:
        drain_blocks(sum_send.at[a], 3 * layers)
    for o in range(1, n):
        pltpu.make_async_remote_copy(
            src_ref=squares.at[me], dst_ref=squares.at[me], send_sem=square_sem.at[0], recv_sem=square_sem.at[1],
            **to(lax.rem(me + o, n))).start()
    for i, ref in ((4, F32), (5, F32), (6, BF16)):
        drain_blocks(load_sem.at[i], len(arrays) * layers * (2 if ref == F32 else 1))
    drain(square_sem.at[1], squares.at[pl.ds(0, n - 1)])
    everyone = squares[0]
    for i in range(1, n):
        everyone = everyone + squares[i]
    everyone = jnp.sum(jnp.sum(everyone, axis=1, keepdims=True), axis=0, keepdims=True)
    count = n * sum(ref.size for ref in m)
    factor = jnp.minimum(1.0, 0.5 * lax.rsqrt(everyone / count + 1e-30))

    def ring(way, a, index, layer, start, size, sem):
        here = new[a].at[layer, block(a, index, start, size), :]
        pltpu.make_async_remote_copy(
            src_ref=here, dst_ref=here, send_sem=ring_send.at[a], recv_sem=sem, **to(side[way])).start()

    def back(a, index, layer, start, size):
        here = new[a].at[layer, block(a, index, start, size), :]
        pltpu.make_async_remote_copy(
            src_ref=here, dst_ref=here, send_sem=back_send.at[a], recv_sem=back_sem.at[a], **to(mate)).start()

    hold(1)
    for k, a, l in head_first:
        for q, start, size in pieces(k, a):
            for way in WAYS:
                layer = way * half + l

                def tile(at, carry):
                    here = (layer, *at(start))
                    gradient = near[a][(0, *here)].astype(F32) * factor
                    mean = 0.9 * m[a][here] + 0.1 * gradient
                    variance = 0.95 * v[a][here] + 0.05 * gradient * gradient
                    weight = own_w[a][here].astype(F32)
                    step = mean * lax.rsqrt(variance + 1e-8) + 0.1 * weight
                    m[a][here] = mean
                    v[a][here] = variance
                    new[a][(layer, *at(me * height[a] + start))] = (weight - 0.02 * step).astype(BF16)
                    return carry

                tiles(a, size, tile, 0)
                ring(way, a, me, layer, start, size, first_sem.at[k])
                back(a, me, layer, start, size)
    for k, a, l in steps:
        for way in WAYS:
            ring(way, a, me, (1 - way) * half + l, 0, height[a], second_sem.at[k])
    source = (mine(left_chip), mine(right_chip))
    for k, a, l in head_first:
        drain(first_sem.at[k], far[a].at[:, l])
        for way in WAYS:
            layer = way * half + l
            if k < final:
                back(a, source[way], layer, 0, height[a])
            else:
                here = new[a].at[layer, block(a, source[way]), :]
                pltpu.make_async_remote_copy(
                    src_ref=here, dst_ref=here, send_sem=tail_sem.at[2], recv_sem=tail_sem.at[way], **to(mate)).start()

    for k, a, l in steps[:final]:
        for way in WAYS:
            here = new[a].at[way * half + l, block(a, source[way]), :]
            there = last.at[way] if k == final - 1 else here
            pltpu.make_async_remote_copy(
                src_ref=here, dst_ref=there, send_sem=ring_send.at[a], recv_sem=last_sem.at[k], **to(side[way])).start()
    for k, a, l in steps:
        drain(second_sem.at[k], far[a].at[:, l])
        for way in WAYS:
            layer = (1 - way) * half + l
            back(a, source[way], layer, 0, height[a])
    _, a, l = steps[final]
    for way in WAYS:
        drain(tail_sem.at[way], new[a].at[way * half + l, block(a, mates((left_chip, right_chip)[way])), :])
    pair = CORES * height[a]
    where = pl.ds(pl.multiple_of((left_chip + core * (right_chip - left_chip)) * pair, pair), pair)
    to_tail = pltpu.make_async_copy(new[a].at[core * half + l, where, :], tail, tail_sem.at[3])
    to_tail.start()
    for k, a, l in steps[: final - 1]:
        drain(last_sem.at[k], far[a].at[:, l])
        for way in WAYS:
            layer = way * half + l
            back(a, mine(far_chip), layer, 0, height[a])
    to_tail.wait()
    drain(tail_sem.at[2], new[fine].at[0, pl.ds(0, 2 * height[fine]), :])
    for a in arrays:
        drain(mate_send.at[a], new[a].at[:half])
        blocks = (4 * layers - (4 if a == fine else 2 if a == steps[final - 1][1] else 0)) // half
        for sem in (back_send, back_sem):
            drain(sem.at[a], new[a].at[:half, pl.ds(0, blocks * height[a]), :])
        drain_blocks(ring_send.at[a], 3 * layers - (2 if a == fine else 0))
    drain(last_sem.at[final - 1], last)
    drain(square_sem.at[0], squares.at[pl.ds(0, n - 1)])


def solution(mesh):
    n = mesh.shape["dp"]
    chips = n // CORES
    onward = [(i, (i // CORES + (1 if i % CORES == 0 else chips - 1)) % chips * CORES + 1 - i % CORES) for i in range(n)]
    mates = [(i, i // CORES * CORES + 1 - i % CORES) for i in range(n)]

    def step(*arrays):
        terms, weights, m, v = (arrays[i : i + 3] for i in (0, 3, 6, 9))
        layers = m[0].shape[0]
        hbm = pl.BlockSpec(memory_space=pltpu.HBM)
        vmem = pl.BlockSpec(memory_space=pltpu.VMEM)
        dma = pltpu.SemaphoreType.DMA
        blocks = [one.shape[1:] for one in m]
        fine = max(range(3), key=lambda a: blocks[a][0])
        out = [(w.shape, BF16) for w in weights] + [(x.shape, F32) for x in (*m, *v)]
        steps = 3 * (layers // 2)
        rows, columns = blocks[fine]
        scratch = (
            [pltpu.VMEM((2, layers // 2, *b), BF16) for b in blocks]
            + [pltpu.VMEM((2, layers, *b), BF16) for b in blocks]
            + [pltpu.VMEM((layers, *b), BF16) for b in blocks]
            + [pltpu.VMEM((layers, *blocks[fine]), BF16), pltpu.VMEM((8, 128), F32), pltpu.VMEM((n, 8, 128), F32)]
            + [dma((7,)), dma((4,)), dma((len(PIECES),)), dma((2,))]
            + [dma((steps,)), dma((steps,)), dma((steps - 1 + len(PIECES),))]
            + [dma((3,)), dma((3,)), dma((3,)), dma((3,)), dma((3,)), dma((2,)), dma((4,))]
        )
        late = [a for a in range(3) if a != fine][-1]
        *results, tail, last = pl.pallas_call(
            functools.partial(kernel, n, fine),
            out_shape=[pltpu.VMEM(shape, dtype) for shape, dtype in [*out, ((CORES * rows, columns), BF16), ((2, *blocks[late]), BF16)]],
            in_specs=[hbm] * len(arrays),
            out_specs=[vmem] * (len(out) + 2),
            scratch_shapes=scratch,
            compiler_params=pltpu.CompilerParams(
                collective_id=0, has_side_effects=True, vmem_limit_bytes=VMEM_LIMIT),
        )(*arrays)

        def write(done, indices, patches=()):
            held = [pltpu.with_memory_space_constraint(x, pltpu.VMEM) for x in (*(results[i] for i in indices), *(p[1] for p in patches))]
            changed = sorted({p[0] for p in patches})
            written = [*changed, *indices]

            def body(*refs):
                olds, refs = refs[: len(changed)], refs[len(changed) :]
                ins, outs, sem = refs[: len(held)], dict(zip(written, refs[len(held) : -1], strict=True)), refs[-1]
                to = [outs[i] for i in indices] + [place(outs[i]) for i, _, place in patches]
                copies = [pltpu.make_async_copy(x, y, sem.at[i]) for i, (x, y) in enumerate(zip(ins, to, strict=True))]
                for copy in copies:
                    copy.start()
                for copy in copies:
                    copy.wait()

            fresh = pl.pallas_call(
                body,
                out_shape=[jax.ShapeDtypeStruct(*out[i]) for i in written],
                in_specs=[hbm] * len(changed) + [vmem] * len(held),
                out_specs=[hbm] * len(written),
                scratch_shapes=[dma((len(held),))],
                input_output_aliases={i: i for i in range(len(changed))},
                compiler_params=pltpu.CompilerParams(vmem_limit_bytes=VMEM_LIMIT),
                cost_estimate=pl.CostEstimate(
                    flops=0, bytes_accessed=2 * sum(x.size * x.dtype.itemsize for x in held), transcendentals=0),
            )(*(done[i] for i in changed), *held)
            done.update(zip(written, fresh, strict=True))

        def far_rows(of_mate):
            me = lax.axis_index("dp")
            core = me % CORES
            return lax.rem(me // CORES + chips // 2, chips), (1 - core if of_mate else core)

        def from_tail(of_mate):
            def place(ref):
                far_chip, core = far_rows(of_mate)
                pair = CORES * rows
                return ref.at[(CORES - core) * (layers // 2) - 1, pl.ds(pl.multiple_of(far_chip * pair, pair), pair), :]

            return place

        def from_last(of_mate):
            def place(ref):
                far_chip, core = far_rows(of_mate)
                size = blocks[late][0]
                return ref.at[layers // 2 - 1 :: layers // 2, pl.ds(pl.multiple_of((far_chip * CORES + core) * size, size), size), :]

            return place

        done = {}
        own = lax.ppermute(tail, "dp", onward)
        mates_last = lax.ppermute(last, "dp", mates)
        write(done, FIRST)
        own, done[fine] = lax.optimization_barrier((own, done[fine]))
        mates_own = lax.ppermute(own, "dp", mates)
        write(done, [i for i in range(9) if i not in FIRST],
              [(fine, own, from_tail(False)), (late, last, from_last(False)), (late, mates_last, from_last(True))])
        write(done, [], [(fine, mates_own, from_tail(True))])
        return tuple(done[i] for i in range(9))

    all_of, cut = P(None, None, None), P(None, "dp", None)
    return jax.shard_map(
        step,
        mesh=mesh,
        in_specs=(P(("rep", "dp"), None, None, None),) * 3 + (all_of,) * 3 + (cut,) * 6,
        out_specs=(P("rep", None, None),) * 3 + (P("rep", "dp", None),) * 6,
        check_vma=False,
    )
```

```python
import functools
import math

import jax
import jax.numpy as jnp
from jax import lax
from jax.experimental import pallas as pl
from jax.experimental.pallas import tpu as pltpu
from jax.sharding import PartitionSpec as P

MESH = pl.DeviceIdType.MESH
CORES = 2
PIECES = (32, 32, 16, 8, 4, 2)
HOLD = ((0, 3000), (1000, 0))
TILE = (16, 512)
WAYS = (0, 1)
F32, BF16 = jnp.float32, jnp.bfloat16
FIRST = range(8)
VMEM_LIMIT = 16 * 2**20


def kernel(n, fine, *refs):
    g, w, m_in, v_in, new, m, v = (refs[i : i + 3] for i in range(0, 21, 3))
    tail, last, *refs = refs[21:]
    far, near, own_w = (refs[i : i + 3] for i in range(0, 9, 3))
    (stage, acc, squares, load_sem, mate_sem, head_sem, stage_sem, first_sem, second_sem, last_sem, back_sem, mate_send,
     back_send, sum_send, ring_send, square_sem, tail_sem) = refs[9:]

    chips = n // CORES
    me = lax.axis_index("dp")
    chip, core = me // CORES, me % CORES
    mate = chip * CORES + 1 - core
    right_chip, left_chip = lax.rem(chip + 1, chips), lax.rem(chip + chips - 1, chips)
    far_chip = lax.rem(chip + 2, chips)
    side = (right_chip * CORES + core, left_chip * CORES + core)
    layers = m[0].shape[0]
    half = layers // 2
    height = [ref.shape[1] for ref in m]
    arrays = [a for a in range(3) if a != fine] + [fine]
    steps = [(k, a, l) for k, (l, a) in enumerate((l, a) for l in range(half) for a in arrays)]
    final = len(steps) - 1
    head_first = steps[final:] + steps[:final]

    def to(device):
        return {"device_id": {"dp": device}, "device_id_type": MESH}

    def mine(c):
        return c * CORES + core

    def mates(c):
        return c * CORES + 1 - core

    def block(a, index, start=0, size=None):
        size = size or height[a]
        return pl.ds(pl.multiple_of(index * height[a] + start, math.gcd(height[a], start)), size)

    def pieces(k, a, order=1):
        sizes = [height[a] // p for p in PIECES[::order]] if k == final else [height[a]]
        return [(q, sum(sizes[:q]), size) for q, size in enumerate(sizes)]

    head = pieces(final, fine)

    def tiles(a, size, body, carry):
        columns = m[a].shape[2] // TILE[1]

        def tile(i, carry):
            def at(base):
                r = pl.multiple_of(base + i // columns * TILE[0], TILE[0])
                return pl.ds(r, TILE[0]), pl.ds(pl.multiple_of(i % columns * TILE[1], TILE[1]), TILE[1])

            return body(at, carry)

        return lax.fori_loop(0, size // TILE[0] * columns, tile, carry)

    def drain(sem, ref):
        pltpu.make_async_copy(ref, ref, sem).wait()

    targets = (far_chip, right_chip, left_chip, chip)

    def group(t, a):
        return (0 if a == fine else 1) if t == 0 else 2 if t < 3 else 3

    def term(t, a):
        where = block(a, mine(targets[t]))
        return pltpu.make_async_copy(g[a].at[0, :, where, :], new[a].at[:, where, :], load_sem.at[group(t, a)])

    def mate_term(t, a):
        return pltpu.make_async_remote_copy(
            src_ref=g[a].at[0, :, block(a, mates(targets[t])), :], dst_ref=new[a].at[:, block(a, mine(targets[t])), :],
            send_sem=mate_send.at[a], recv_sem=mate_sem.at[group(t, a)], **to(mate))

    def mate_head(q, start, size):
        return pltpu.make_async_remote_copy(
            src_ref=stage.at[:, pl.ds(start, size), :],
            dst_ref=new[fine].at[:, block(fine, mine(far_chip), start, size), :],
            send_sem=mate_send.at[fine], recv_sem=head_sem.at[q], **to(mate))

    def to_stage(q, start, size):
        return pltpu.make_async_copy(
            g[fine].at[0, :, block(fine, mates(far_chip), start, size), :], stage.at[:, pl.ds(start, size), :], stage_sem.at[q])

    staged = [(0, *head[0][1:]), (1, head[1][1], height[fine] - head[1][1])]

    def states(a):
        return (pltpu.make_async_copy(m_in[a], m[a], load_sem.at[4]),
                pltpu.make_async_copy(v_in[a], v[a], load_sem.at[5]),
                pltpu.make_async_copy(w[a].at[:, block(a, me), :], own_w[a], load_sem.at[6]))

    for q, start, size in staged:
        to_stage(q, start, size).start()
    barrier = pltpu.get_barrier_semaphore()
    for o in range(1, n):
        pl.semaphore_signal(barrier, inc=1, **to(lax.rem(me + o, n)))
    for a in (fine, *arrays[:-1]):
        term(0, a).start()
    to_stage(*staged[0]).wait()
    pl.semaphore_wait(barrier, n - 1)
    mate_head(*head[0]).start()
    to_stage(*staged[1]).wait()
    for piece in head[1:]:
        mate_head(*piece).start()
    for t, a in [(0, a) for a in arrays[:-1]] + [(t, a) for a in arrays for t in (1, 2)] + [(3, a) for a in arrays]:
        mate_term(t, a).start()
        if t > 0:
            term(t, a).start()
    for a in arrays:
        for copy in states(a):
            copy.start()
    acc[...] = jnp.zeros_like(acc)

    def drain_blocks(sem, count):
        drain(sem, new[fine].at[:, pl.ds(0, count * height[fine] // layers), :])

    arrived = set()

    def await_terms(t, a):
        i = group(t, a)
        if i not in arrived:
            arrived.add(i)
            count = layers * sum(group(t, a) == i for t in range(4) for a in arrays)
            drain_blocks(load_sem.at[i], count)
            if i > 0:
                drain_blocks(mate_sem.at[i], count)

    def total(t, a, layer, at, start, more):
        out = new[a][(layer, *at(mine(targets[t]) * height[a] + start))].astype(F32)
        out = out + new[a][(layer, *at(mates(targets[t]) * height[a] + start))].astype(F32)
        for ref, index in more:
            out = out + ref[(*index, *at(start))].astype(F32)
        return out

    def summed(t, a, layer, start, size, more=()):
        def tile(at, carry):
            new[a][(layer, *at(mine(targets[t]) * height[a] + start))] = total(t, a, layer, at, start, more).astype(BF16)
            return carry

        tiles(a, size, tile, 0)
        return new[a].at[layer, block(a, mine(targets[t]), start, size), :]

    def send_sum(way, a, src, dst, sem):
        pltpu.make_async_remote_copy(
            src_ref=src, dst_ref=dst, send_sem=sum_send.at[a], recv_sem=sem, **to(side[way])).start()

    def hold(phase):
        for index, time in enumerate(HOLD[phase]):
            if time:
                pl.when(core == index)(lambda: pl.delay(time))

    hold(0)
    for k, a, l in head_first:
        await_terms(0, a)
        for q, start, size in pieces(k, a):
            if a == fine and k == final:
                mate_head(q, start, size).wait_recv()
            for way in WAYS:
                src = summed(0, a, way * half + l, start, size)
                send_sum(way, a, src, far[a].at[way, l, pl.ds(start, size), :], first_sem.at[k])
    for k, a, l in steps:
        for way in WAYS:
            await_terms(1 + way, a)
            layer = (1 - way) * half + l
            src = summed(1 + way, a, layer, 0, height[a])
            send_sum(way, a, src, near[a].at[way, layer], second_sem.at[k])
    for k, a, l in steps:
        drain(first_sem.at[k], far[a].at[:, l])
        for q, start, size in pieces(k, a, -1):
            for way in WAYS:
                layer = way * half + l
                src = summed(1 + way, a, layer, start, size, [(far[a], (way, l))])
                send_sum(way, a, src, near[a].at[way, layer, pl.ds(start, size), :], last_sem.at[k + q])
    for k, a, l in steps:
        await_terms(3, a)
        drain(second_sem.at[k], far[a].at[:, l])
        for q, start, size in pieces(k, a, -1):
            drain(last_sem.at[k + q], far[a].at[:, l, pl.ds(start, size), :])
            for way in WAYS:
                layer = way * half + l

                def tile(at, carry):
                    rounded = total(3, a, layer, at, start, [(near[a], (i, layer)) for i in WAYS]).astype(BF16)
                    near[a][(0, layer, *at(start))] = rounded
                    rounded = rounded.astype(F32)
                    square = rounded * rounded
                    for r in range(0, TILE[0], 8):
                        for c in range(0, TILE[1], 128):
                            carry = carry + square[r : r + 8, c : c + 128]
                    return carry

                acc[...] = tiles(a, size, tile, acc[...])

    squares[me] = jnp.sum(acc[...], axis=0, keepdims=True)
    for a in arrays:
        drain_blocks(sum_send.at[a], 3 * layers)
    for o in range(1, n):
        pltpu.make_async_remote_copy(
            src_ref=squares.at[me], dst_ref=squares.at[me], send_sem=square_sem.at[0], recv_sem=square_sem.at[1],
            **to(lax.rem(me + o, n))).start()
    for i, ref in ((4, F32), (5, F32), (6, BF16)):
        drain_blocks(load_sem.at[i], len(arrays) * layers * (2 if ref == F32 else 1))
    drain(square_sem.at[1], squares.at[pl.ds(0, n - 1)])
    everyone = squares[0]
    for i in range(1, n):
        everyone = everyone + squares[i]
    everyone = jnp.sum(everyone, axis=1, keepdims=True)
    count = n * sum(ref.size for ref in m)
    factor = jnp.minimum(1.0, 0.5 * lax.rsqrt(everyone / count + 1e-30))

    def ring(way, a, index, layer, start, size, sem):
        here = new[a].at[layer, block(a, index, start, size), :]
        pltpu.make_async_remote_copy(
            src_ref=here, dst_ref=here, send_sem=ring_send.at[a], recv_sem=sem, **to(side[way])).start()

    def back(a, index, layer, start, size):
        here = new[a].at[layer, block(a, index, start, size), :]
        pltpu.make_async_remote_copy(
            src_ref=here, dst_ref=here, send_sem=back_send.at[a], recv_sem=back_sem.at[a], **to(mate)).start()

    hold(1)
    for k, a, l in head_first:
        for q, start, size in pieces(k, a):
            for way in WAYS:
                layer = way * half + l

                def tile(at, carry):
                    here = (layer, *at(start))
                    gradient = near[a][(0, *here)].astype(F32) * factor
                    mean = 0.9 * m[a][here] + 0.1 * gradient
                    variance = 0.95 * v[a][here] + 0.05 * gradient * gradient
                    weight = own_w[a][here].astype(F32)
                    step = mean * lax.rsqrt(variance + 1e-8) + 0.1 * weight
                    m[a][here] = mean
                    v[a][here] = variance
                    new[a][(layer, *at(me * height[a] + start))] = (weight - 0.02 * step).astype(BF16)
                    return carry

                tiles(a, size, tile, 0)
                ring(way, a, me, layer, start, size, first_sem.at[k])
                back(a, me, layer, start, size)
    for k, a, l in steps:
        for way in WAYS:
            ring(way, a, me, (1 - way) * half + l, 0, height[a], second_sem.at[k])
    source = (mine(left_chip), mine(right_chip))
    for k, a, l in head_first:
        drain(first_sem.at[k], far[a].at[:, l])
        for way in WAYS:
            layer = way * half + l
            if k < final:
                back(a, source[way], layer, 0, height[a])
            else:
                here = new[a].at[layer, block(a, source[way]), :]
                pltpu.make_async_remote_copy(
                    src_ref=here, dst_ref=here, send_sem=tail_sem.at[2], recv_sem=tail_sem.at[way], **to(mate)).start()

    for k, a, l in steps[:final]:
        for way in WAYS:
            here = new[a].at[way * half + l, block(a, source[way]), :]
            there, device = (here, side[way]) if k < final - 1 else (last.at[way], side[way] + 1 - 2 * core)
            pltpu.make_async_remote_copy(
                src_ref=here, dst_ref=there, send_sem=ring_send.at[a], recv_sem=last_sem.at[k], **to(device)).start()
    for k, a, l in steps:
        drain(second_sem.at[k], far[a].at[:, l])
        for way in WAYS:
            layer = (1 - way) * half + l
            back(a, source[way], layer, 0, height[a])
    _, a, l = steps[final]
    for way in WAYS:
        drain(tail_sem.at[way], new[a].at[way * half + l, block(a, mates((left_chip, right_chip)[way])), :])
    pair = CORES * height[a]
    where = pl.ds(pl.multiple_of((right_chip + core * (left_chip - right_chip)) * pair, pair), pair)
    to_tail = pltpu.make_async_copy(new[a].at[(1 - core) * half + l, where, :], tail, tail_sem.at[3])
    to_tail.start()
    for k, a, l in steps[: final - 1]:
        drain(last_sem.at[k], far[a].at[:, l])
        for way in WAYS:
            layer = way * half + l
            back(a, mine(far_chip), layer, 0, height[a])
    to_tail.wait()
    drain(tail_sem.at[2], new[fine].at[0, pl.ds(0, 2 * height[fine]), :])
    for a in arrays:
        drain(mate_send.at[a], new[a].at[:half])
        blocks = (4 * layers - (4 if a == fine else 2 if a == steps[final - 1][1] else 0)) // half
        for sem in (back_send, back_sem):
            drain(sem.at[a], new[a].at[:half, pl.ds(0, blocks * height[a]), :])
        drain_blocks(ring_send.at[a], 3 * layers - (2 if a == fine else 0))
    drain(last_sem.at[final - 1], last)
    drain(square_sem.at[0], squares.at[pl.ds(0, n - 1)])


def solution(mesh):
    n = mesh.shape["dp"]
    chips = n // CORES
    onward = [(i, (i // CORES + (chips - 1 if i % CORES == 0 else 1)) % chips * CORES + 1 - i % CORES) for i in range(n)]
    mates = [(i, i // CORES * CORES + 1 - i % CORES) for i in range(n)]

    def step(*arrays):
        terms, weights, m, v = (arrays[i : i + 3] for i in (0, 3, 6, 9))
        layers = m[0].shape[0]
        hbm = pl.BlockSpec(memory_space=pltpu.HBM)
        vmem = pl.BlockSpec(memory_space=pltpu.VMEM)
        dma = pltpu.SemaphoreType.DMA
        blocks = [one.shape[1:] for one in m]
        fine = max(range(3), key=lambda a: blocks[a][0])
        out = [(w.shape, BF16) for w in weights] + [(x.shape, F32) for x in (*m, *v)]
        steps = 3 * (layers // 2)
        rows, columns = blocks[fine]
        scratch = (
            [pltpu.VMEM((2, layers // 2, *b), BF16) for b in blocks]
            + [pltpu.VMEM((2, layers, *b), BF16) for b in blocks]
            + [pltpu.VMEM((layers, *b), BF16) for b in blocks]
            + [pltpu.VMEM((layers, *blocks[fine]), BF16), pltpu.VMEM((8, 128), F32), pltpu.VMEM((n, 1, 128), F32)]
            + [dma((7,)), dma((4,)), dma((len(PIECES),)), dma((2,))]
            + [dma((steps,)), dma((steps,)), dma((steps - 1 + len(PIECES),))]
            + [dma((3,)), dma((3,)), dma((3,)), dma((3,)), dma((3,)), dma((2,)), dma((4,))]
        )
        late = [a for a in range(3) if a != fine][-1]
        *results, tail, last = pl.pallas_call(
            functools.partial(kernel, n, fine),
            out_shape=[pltpu.VMEM(shape, dtype) for shape, dtype in [*out, ((CORES * rows, columns), BF16), ((2, *blocks[late]), BF16)]],
            in_specs=[hbm] * len(arrays),
            out_specs=[vmem] * (len(out) + 2),
            scratch_shapes=scratch,
            compiler_params=pltpu.CompilerParams(
                collective_id=0, has_side_effects=True, vmem_limit_bytes=VMEM_LIMIT),
        )(*arrays)

        def write(done, indices, patches=()):
            held = [pltpu.with_memory_space_constraint(x, pltpu.VMEM) for x in (*(results[i] for i in indices), *(p[1] for p in patches))]
            changed = sorted({p[0] for p in patches})
            written = [*changed, *indices]

            def body(*refs):
                olds, refs = refs[: len(changed)], refs[len(changed) :]
                ins, outs, sem = refs[: len(held)], dict(zip(written, refs[len(held) : -1], strict=True)), refs[-1]
                to = [outs[i] for i in indices] + [place(outs[i]) for i, _, place in patches]
                copies = [pltpu.make_async_copy(x, y, sem.at[i]) for i, (x, y) in enumerate(zip(ins, to, strict=True))]
                for copy in copies:
                    copy.start()
                for copy in copies:
                    copy.wait()

            fresh = pl.pallas_call(
                body,
                out_shape=[jax.ShapeDtypeStruct(*out[i]) for i in written],
                in_specs=[hbm] * len(changed) + [vmem] * len(held),
                out_specs=[hbm] * len(written),
                scratch_shapes=[dma((len(held),))],
                input_output_aliases={i: i for i in range(len(changed))},
                compiler_params=pltpu.CompilerParams(vmem_limit_bytes=VMEM_LIMIT),
                cost_estimate=pl.CostEstimate(
                    flops=0, bytes_accessed=2 * sum(x.size * x.dtype.itemsize for x in held), transcendentals=0),
            )(*(done[i] for i in changed), *held)
            done.update(zip(written, fresh, strict=True))

        def far_rows(of_mate):
            me = lax.axis_index("dp")
            core = me % CORES
            return lax.rem(me // CORES + chips // 2, chips), (1 - core if of_mate else core)

        def from_tail(of_mate):
            def place(ref):
                far_chip, core = far_rows(of_mate)
                pair = CORES * rows
                return ref.at[(core + 1) * (layers // 2) - 1, pl.ds(pl.multiple_of(far_chip * pair, pair), pair), :]

            return place

        def from_last(of_mate):
            def place(ref):
                far_chip, core = far_rows(not of_mate)
                size = blocks[late][0]
                return ref.at[layers // 2 - 1 :: layers // 2, pl.ds(pl.multiple_of((far_chip * CORES + core) * size, size), size), :]

            return place

        done = {}
        own = lax.ppermute(tail, "dp", onward)
        mates_last = lax.ppermute(last, "dp", mates)
        write(done, FIRST)
        own, done[fine] = lax.optimization_barrier((own, done[fine]))
        mates_own = lax.ppermute(own, "dp", mates)
        write(done, [i for i in range(9) if i not in FIRST],
              [(fine, own, from_tail(False)), (late, last, from_last(False)), (late, mates_last, from_last(True))])
        write(done, [], [(fine, mates_own, from_tail(True))])
        return tuple(done[i] for i in range(9))

    all_of, cut = P(None, None, None), P(None, "dp", None)
    return jax.shard_map(
        step,
        mesh=mesh,
        in_specs=(P(("rep", "dp"), None, None, None),) * 3 + (all_of,) * 3 + (cut,) * 6,
        out_specs=(P("rep", None, None),) * 3 + (P("rep", "dp", None),) * 6,
        check_vma=False,
    )
```

```python
import functools
import math

import jax
import jax.numpy as jnp
from jax import lax
from jax.experimental import pallas as pl
from jax.experimental.pallas import tpu as pltpu
from jax.sharding import PartitionSpec as P

MESH = pl.DeviceIdType.MESH
CORES = 2
PIECES = (32, 32, 16, 8, 4, 2)
HOLD = ((0, 3000), (1000, 0))
TILE = (16, 512)
WAYS = (0, 1)
F32, BF16 = jnp.float32, jnp.bfloat16
FIRST = range(8)
VMEM_LIMIT = 16 * 2**20


def kernel(n, fine, *refs):
    g, w, m_in, v_in, new, m, v = (refs[i : i + 3] for i in range(0, 21, 3))
    tail, last, *refs = refs[21:]
    far, near, own_w = (refs[i : i + 3] for i in range(0, 9, 3))
    (stage, acc, squares, load_sem, mate_sem, head_sem, stage_sem, first_sem, second_sem, last_sem, back_sem, mate_send,
     back_send, sum_send, ring_send, square_sem, tail_sem) = refs[9:]

    chips = n // CORES
    me = lax.axis_index("dp")
    chip, core = me // CORES, me % CORES
    mate = chip * CORES + 1 - core
    right_chip, left_chip = lax.rem(chip + 1, chips), lax.rem(chip + chips - 1, chips)
    far_chip = lax.rem(chip + 2, chips)
    side = (right_chip * CORES + core, left_chip * CORES + core)
    layers = m[0].shape[0]
    half = layers // 2
    height = [ref.shape[1] for ref in m]
    arrays = [a for a in range(3) if a != fine] + [fine]
    steps = [(k, a, l) for k, (l, a) in enumerate((l, a) for l in range(half) for a in arrays)]
    final = len(steps) - 1
    head_first = steps[final:] + steps[:final]

    def to(device):
        return {"device_id": {"dp": device}, "device_id_type": MESH}

    def mine(c):
        return c * CORES + core

    def mates(c):
        return c * CORES + 1 - core

    def block(a, index, start=0, size=None):
        size = size or height[a]
        return pl.ds(pl.multiple_of(index * height[a] + start, math.gcd(height[a], start)), size)

    def pieces(k, a, order=1):
        sizes = [height[a] // p for p in PIECES[::order]] if k == final else [height[a]]
        return [(q, sum(sizes[:q]), size) for q, size in enumerate(sizes)]

    head = pieces(final, fine)

    def tiles(a, size, body, carry):
        columns = m[a].shape[2] // TILE[1]

        def tile(i, carry):
            def at(base):
                r = pl.multiple_of(base + i // columns * TILE[0], TILE[0])
                return pl.ds(r, TILE[0]), pl.ds(pl.multiple_of(i % columns * TILE[1], TILE[1]), TILE[1])

            return body(at, carry)

        return lax.fori_loop(0, size // TILE[0] * columns, tile, carry)

    def drain(sem, ref):
        pltpu.make_async_copy(ref, ref, sem).wait()

    targets = (far_chip, right_chip, left_chip, chip)

    def group(t, a):
        return (0 if a == fine else 1) if t == 0 else 2 if t < 3 else 3

    def term(t, a):
        where = block(a, mine(targets[t]))
        return pltpu.make_async_copy(g[a].at[0, :, where, :], new[a].at[:, where, :], load_sem.at[group(t, a)])

    def mate_term(t, a):
        return pltpu.make_async_remote_copy(
            src_ref=g[a].at[0, :, block(a, mates(targets[t])), :], dst_ref=new[a].at[:, block(a, mine(targets[t])), :],
            send_sem=mate_send.at[a], recv_sem=mate_sem.at[group(t, a)], **to(mate))

    def mate_head(q, start, size):
        return pltpu.make_async_remote_copy(
            src_ref=stage.at[:, pl.ds(start, size), :],
            dst_ref=new[fine].at[:, block(fine, mine(far_chip), start, size), :],
            send_sem=mate_send.at[fine], recv_sem=head_sem.at[q], **to(mate))

    def to_stage(q, start, size):
        return pltpu.make_async_copy(
            g[fine].at[0, :, block(fine, mates(far_chip), start, size), :], stage.at[:, pl.ds(start, size), :], stage_sem.at[q])

    staged = [(0, *head[0][1:]), (1, head[1][1], height[fine] - head[1][1])]

    def states(a):
        return (pltpu.make_async_copy(m_in[a], m[a], load_sem.at[4]),
                pltpu.make_async_copy(v_in[a], v[a], load_sem.at[5]),
                pltpu.make_async_copy(w[a].at[:, block(a, me), :], own_w[a], load_sem.at[6]))

    for q, start, size in staged:
        to_stage(q, start, size).start()
    barrier = pltpu.get_barrier_semaphore()
    for o in range(1, n):
        pl.semaphore_signal(barrier, inc=1, **to(lax.rem(me + o, n)))
    term(0, fine).start()
    to_stage(*staged[0]).wait()
    pl.semaphore_wait(barrier, n - 1)
    mate_head(*head[0]).start()
    for a in arrays[:-1]:
        term(0, a).start()
    to_stage(*staged[1]).wait()
    for piece in head[1:]:
        mate_head(*piece).start()
    for t, a in [(0, a) for a in arrays[:-1]] + [(t, a) for a in arrays for t in (1, 2)] + [(3, a) for a in arrays]:
        mate_term(t, a).start()
        if t > 0:
            term(t, a).start()
    for a in arrays:
        for copy in states(a):
            copy.start()
    acc[...] = jnp.zeros_like(acc)

    def drain_blocks(sem, count):
        drain(sem, new[fine].at[:, pl.ds(0, count * height[fine] // layers), :])

    arrived = set()

    def await_terms(t, a):
        i = group(t, a)
        if i not in arrived:
            arrived.add(i)
            count = layers * sum(group(t, a) == i for t in range(4) for a in arrays)
            drain_blocks(load_sem.at[i], count)
            if i > 0:
                drain_blocks(mate_sem.at[i], count)

    def total(t, a, layer, at, start, more):
        out = new[a][(layer, *at(mine(targets[t]) * height[a] + start))].astype(F32)
        out = out + new[a][(layer, *at(mates(targets[t]) * height[a] + start))].astype(F32)
        for ref, index in more:
            out = out + ref[(*index, *at(start))].astype(F32)
        return out

    def summed(t, a, layer, start, size, more=()):
        def tile(at, carry):
            new[a][(layer, *at(mine(targets[t]) * height[a] + start))] = total(t, a, layer, at, start, more).astype(BF16)
            return carry

        tiles(a, size, tile, 0)
        return new[a].at[layer, block(a, mine(targets[t]), start, size), :]

    def send_sum(way, a, src, dst, sem):
        pltpu.make_async_remote_copy(
            src_ref=src, dst_ref=dst, send_sem=sum_send.at[a], recv_sem=sem, **to(side[way])).start()

    def hold(phase):
        for index, time in enumerate(HOLD[phase]):
            if time:
                pl.when(core == index)(lambda: pl.delay(time))

    hold(0)
    for k, a, l in head_first:
        await_terms(0, a)
        for q, start, size in pieces(k, a):
            if a == fine and k == final:
                mate_head(q, start, size).wait_recv()
            for way in WAYS:
                src = summed(0, a, way * half + l, start, size)
                send_sum(way, a, src, far[a].at[way, l, pl.ds(start, size), :], first_sem.at[k])
    for k, a, l in steps:
        for way in WAYS:
            await_terms(1 + way, a)
            layer = (1 - way) * half + l
            src = summed(1 + way, a, layer, 0, height[a])
            send_sum(way, a, src, near[a].at[way, layer], second_sem.at[k])
    for k, a, l in steps:
        drain(first_sem.at[k], far[a].at[:, l])
        for q, start, size in pieces(k, a, -1):
            for way in WAYS:
                layer = way * half + l
                src = summed(1 + way, a, layer, start, size, [(far[a], (way, l))])
                send_sum(way, a, src, near[a].at[way, layer, pl.ds(start, size), :], last_sem.at[k + q])
    for k, a, l in steps:
        await_terms(3, a)
        drain(second_sem.at[k], far[a].at[:, l])
        for q, start, size in pieces(k, a, -1):
            drain(last_sem.at[k + q], far[a].at[:, l, pl.ds(start, size), :])
            for way in WAYS:
                layer = way * half + l

                def tile(at, carry):
                    rounded = total(3, a, layer, at, start, [(near[a], (i, layer)) for i in WAYS]).astype(BF16)
                    near[a][(0, layer, *at(start))] = rounded
                    rounded = rounded.astype(F32)
                    square = rounded * rounded
                    for r in range(0, TILE[0], 8):
                        for c in range(0, TILE[1], 128):
                            carry = carry + square[r : r + 8, c : c + 128]
                    return carry

                acc[...] = tiles(a, size, tile, acc[...])

    squares[me] = jnp.sum(acc[...], axis=0, keepdims=True)
    for a in arrays:
        drain_blocks(sum_send.at[a], 3 * layers)
    for o in range(1, n):
        pltpu.make_async_remote_copy(
            src_ref=squares.at[me], dst_ref=squares.at[me], send_sem=square_sem.at[0], recv_sem=square_sem.at[1],
            **to(lax.rem(me + o, n))).start()
    for i, ref in ((4, F32), (5, F32), (6, BF16)):
        drain_blocks(load_sem.at[i], len(arrays) * layers * (2 if ref == F32 else 1))
    drain(square_sem.at[1], squares.at[pl.ds(0, n - 1)])
    everyone = squares[0]
    for i in range(1, n):
        everyone = everyone + squares[i]
    everyone = jnp.sum(everyone, axis=1, keepdims=True)
    count = n * sum(ref.size for ref in m)
    factor = jnp.minimum(1.0, 0.5 * lax.rsqrt(everyone / count + 1e-30))

    def ring(way, a, index, layer, start, size, sem):
        here = new[a].at[layer, block(a, index, start, size), :]
        pltpu.make_async_remote_copy(
            src_ref=here, dst_ref=here, send_sem=ring_send.at[0], recv_sem=sem, **to(side[way])).start()

    def back(a, index, layer, start, size):
        here = new[a].at[layer, block(a, index, start, size), :]
        pltpu.make_async_remote_copy(
            src_ref=here, dst_ref=here, send_sem=back_send.at[a], recv_sem=back_sem.at[a], **to(mate)).start()

    hold(1)
    for k, a, l in head_first:
        for q, start, size in pieces(k, a):
            for way in WAYS:
                layer = way * half + l

                def tile(at, carry):
                    here = (layer, *at(start))
                    gradient = near[a][(0, *here)].astype(F32) * factor
                    mean = 0.9 * m[a][here] + 0.1 * gradient
                    variance = 0.95 * v[a][here] + 0.05 * gradient * gradient
                    weight = own_w[a][here].astype(F32)
                    step = mean * lax.rsqrt(variance + 1e-8) + 0.1 * weight
                    m[a][here] = mean
                    v[a][here] = variance
                    new[a][(layer, *at(me * height[a] + start))] = (weight - 0.02 * step).astype(BF16)
                    return carry

                tiles(a, size, tile, 0)
                ring(way, a, me, layer, start, size, first_sem.at[k])
                back(a, me, layer, start, size)
    for k, a, l in steps:
        for way in WAYS:
            ring(way, a, me, (1 - way) * half + l, 0, height[a], second_sem.at[k])
    source = (mine(left_chip), mine(right_chip))
    for k, a, l in head_first:
        drain(first_sem.at[k], far[a].at[:, l])
        for way in WAYS:
            layer = way * half + l
            if k < final:
                back(a, source[way], layer, 0, height[a])
            else:
                here = new[a].at[layer, block(a, source[way]), :]
                pltpu.make_async_remote_copy(
                    src_ref=here, dst_ref=here, send_sem=tail_sem.at[2], recv_sem=tail_sem.at[way], **to(mate)).start()

    for k, a, l in steps[:final]:
        for way in WAYS:
            here = new[a].at[way * half + l, block(a, source[way]), :]
            there, device = (here, side[way]) if k < final - 1 else (last.at[way], side[way] + 1 - 2 * core)
            pltpu.make_async_remote_copy(
                src_ref=here, dst_ref=there, send_sem=ring_send.at[0], recv_sem=last_sem.at[k], **to(device)).start()
    for k, a, l in steps:
        drain(second_sem.at[k], far[a].at[:, l])
        for way in WAYS:
            layer = (1 - way) * half + l
            back(a, source[way], layer, 0, height[a])
    _, a, l = steps[final]
    for way in WAYS:
        drain(tail_sem.at[way], new[a].at[way * half + l, block(a, mates((left_chip, right_chip)[way])), :])
    pair = CORES * height[a]
    where = pl.ds(pl.multiple_of((right_chip + core * (left_chip - right_chip)) * pair, pair), pair)
    to_tail = pltpu.make_async_copy(new[a].at[(1 - core) * half + l, where, :], tail, tail_sem.at[3])
    to_tail.start()
    for k, a, l in steps[: final - 1]:
        drain(last_sem.at[k], far[a].at[:, l])
        for way in WAYS:
            layer = way * half + l
            back(a, mine(far_chip), layer, 0, height[a])
    to_tail.wait()
    drain(tail_sem.at[2], new[fine].at[0, pl.ds(0, 2 * height[fine]), :])
    for a in arrays:
        drain(mate_send.at[a], new[a].at[:half])
        blocks = (4 * layers - (4 if a == fine else 2 if a == steps[final - 1][1] else 0)) // half
        for sem in (back_send, back_sem):
            drain(sem.at[a], new[a].at[:half, pl.ds(0, blocks * height[a]), :])
    drain_blocks(ring_send.at[0], 3 * layers * len(arrays) - 2)
    drain(last_sem.at[final - 1], last)
    drain(square_sem.at[0], squares.at[pl.ds(0, n - 1)])


def solution(mesh):
    n = mesh.shape["dp"]
    chips = n // CORES
    onward = [(i, (i // CORES + (chips - 1 if i % CORES == 0 else 1)) % chips * CORES + 1 - i % CORES) for i in range(n)]
    mates = [(i, i // CORES * CORES + 1 - i % CORES) for i in range(n)]

    def step(*arrays):
        terms, weights, m, v = (arrays[i : i + 3] for i in (0, 3, 6, 9))
        layers = m[0].shape[0]
        hbm = pl.BlockSpec(memory_space=pltpu.HBM)
        vmem = pl.BlockSpec(memory_space=pltpu.VMEM)
        dma = pltpu.SemaphoreType.DMA
        blocks = [one.shape[1:] for one in m]
        fine = max(range(3), key=lambda a: blocks[a][0])
        out = [(w.shape, BF16) for w in weights] + [(x.shape, F32) for x in (*m, *v)]
        steps = 3 * (layers // 2)
        rows, columns = blocks[fine]
        scratch = (
            [pltpu.VMEM((2, layers // 2, *b), BF16) for b in blocks]
            + [pltpu.VMEM((2, layers, *b), BF16) for b in blocks]
            + [pltpu.VMEM((layers, *b), BF16) for b in blocks]
            + [pltpu.VMEM((layers, *blocks[fine]), BF16), pltpu.VMEM((8, 128), F32), pltpu.VMEM((n, 1, 128), F32)]
            + [dma((7,)), dma((4,)), dma((len(PIECES),)), dma((2,))]
            + [dma((steps,)), dma((steps,)), dma((steps - 1 + len(PIECES),))]
            + [dma((3,)), dma((3,)), dma((3,)), dma((3,)), dma((1,)), dma((2,)), dma((4,))]
        )
        late = [a for a in range(3) if a != fine][-1]
        *results, tail, last = pl.pallas_call(
            functools.partial(kernel, n, fine),
            out_shape=[pltpu.VMEM(shape, dtype) for shape, dtype in [*out, ((CORES * rows, columns), BF16), ((2, *blocks[late]), BF16)]],
            in_specs=[hbm] * len(arrays),
            out_specs=[vmem] * (len(out) + 2),
            scratch_shapes=scratch,
            compiler_params=pltpu.CompilerParams(
                collective_id=0, has_side_effects=True, vmem_limit_bytes=VMEM_LIMIT),
        )(*arrays)

        def write(done, indices, patches=()):
            held = [pltpu.with_memory_space_constraint(x, pltpu.VMEM) for x in (*(results[i] for i in indices), *(p[1] for p in patches))]
            changed = sorted({p[0] for p in patches})
            written = [*changed, *indices]

            def body(*refs):
                olds, refs = refs[: len(changed)], refs[len(changed) :]
                ins, outs, sem = refs[: len(held)], dict(zip(written, refs[len(held) : -1], strict=True)), refs[-1]
                to = [outs[i] for i in indices] + [place(outs[i]) for i, _, place in patches]
                copies = [pltpu.make_async_copy(x, y, sem.at[i]) for i, (x, y) in enumerate(zip(ins, to, strict=True))]
                for copy in copies:
                    copy.start()
                for copy in copies:
                    copy.wait()

            fresh = pl.pallas_call(
                body,
                out_shape=[jax.ShapeDtypeStruct(*out[i]) for i in written],
                in_specs=[hbm] * len(changed) + [vmem] * len(held),
                out_specs=[hbm] * len(written),
                scratch_shapes=[dma((len(held),))],
                input_output_aliases={i: i for i in range(len(changed))},
                compiler_params=pltpu.CompilerParams(vmem_limit_bytes=VMEM_LIMIT),
                cost_estimate=pl.CostEstimate(
                    flops=0, bytes_accessed=2 * sum(x.size * x.dtype.itemsize for x in held), transcendentals=0),
            )(*(done[i] for i in changed), *held)
            done.update(zip(written, fresh, strict=True))

        def far_rows(of_mate):
            me = lax.axis_index("dp")
            core = me % CORES
            return lax.rem(me // CORES + chips // 2, chips), (1 - core if of_mate else core)

        def from_tail(of_mate):
            def place(ref):
                far_chip, core = far_rows(of_mate)
                pair = CORES * rows
                return ref.at[(core + 1) * (layers // 2) - 1, pl.ds(pl.multiple_of(far_chip * pair, pair), pair), :]

            return place

        def from_last(of_mate):
            def place(ref):
                far_chip, core = far_rows(not of_mate)
                size = blocks[late][0]
                return ref.at[layers // 2 - 1 :: layers // 2, pl.ds(pl.multiple_of((far_chip * CORES + core) * size, size), size), :]

            return place

        done = {}
        own = lax.ppermute(tail, "dp", onward)
        mates_last = lax.ppermute(last, "dp", mates)
        write(done, FIRST)
        own, done[fine] = lax.optimization_barrier((own, done[fine]))
        mates_own = lax.ppermute(own, "dp", mates)
        write(done, [i for i in range(9) if i not in FIRST],
              [(fine, own, from_tail(False)), (late, last, from_last(False)), (late, mates_last, from_last(True))])
        write(done, [], [(fine, mates_own, from_tail(True))])
        return tuple(done[i] for i in range(9))

    all_of, cut = P(None, None, None), P(None, "dp", None)
    return jax.shard_map(
        step,
        mesh=mesh,
        in_specs=(P(("rep", "dp"), None, None, None),) * 3 + (all_of,) * 3 + (cut,) * 6,
        out_specs=(P("rep", None, None),) * 3 + (P("rep", "dp", None),) * 6,
        check_vma=False,
    )
```
